128 devices in a mesh: row: 8 (over y, z_lo), col: 16 (over x, z_hi, core).
Axes of the slice: x: 4, y: 4, z: 4 (z_hi: 2, z_lo: 2; z = z_hi * 2 + z_lo), core: 2. Of those that a mesh axis runs over, the one named last changes fastest.
Arguments:
- view_one: bfloat16 [4096, 8192], P('row', 'col'), may hold values from -6 to 6
- view_two: bfloat16 [4096, 8192], P('row', 'col'), may hold values from -6 to 6
- pair_weights: bfloat16 [8192, 8192], P('row', 'col'), may hold values from 0.25 to 2.5
Outputs:
- first_grad: bfloat16 [4096, 8192], P('row', 'col')
- second_grad: bfloat16 [4096, 8192], P('row', 'col')
The draws below stay inside these ranges and needn't reach their ends.
All inputs are finite; a program needn't handle non-finite values.
Results may differ from the reference program's by a relative error of at most 0.004.
Values may be sent and summed in bfloat16 or wider, within the bound.
A program may use at most 128 MiB of HBM per device.

```python
import math
import jax
import jax.numpy as jnp

D = 8192
BATCH = 4096


def block_levels(own_key, shape, shards, least, high):
    factor_of, own = 1.0, jax.random.fold_in(own_key, 6)
    for position, shards_of in shards:
        heights = jnp.exp(jax.random.uniform(jax.random.fold_in(own, position), (shards_of,), jnp.float32, least / len(shards), high / len(shards)))
        factor_of = factor_of * jnp.repeat(heights, shape[position] // shards_of).reshape([-1 if axis == position else 1 for axis in range(len(shape))])
    return factor_of


def centred(key, shape, scale, bound, cuts=(), held_as=jnp.bfloat16):
    drawn = scale * jax.random.normal(key, shape, jnp.float32)
    if cuts:
        drawn = drawn * block_levels(key, shape, cuts, -0.22, 0.18)
    return jnp.clip(drawn, -bound, bound).astype(held_as)


def setup_inputs(seed: int = 0) -> dict:
    seeds = jax.random.split(jax.random.key(seed), 4)
    return {
        "view_one": centred(seeds[0], (BATCH, D), 1.0, 6.0, ((0, 8), (1, 16))),
        "view_two": centred(seeds[1], (BATCH, D), 1.0, 6.0, ((0, 8), (1, 16))),
        "pair_weights": jnp.clip(jnp.exp(math.log(2.5) - 2.3025851 * jax.random.uniform(seeds[2], (D, D), jnp.float32) ** block_levels(seeds[2], (D, D), ((0, 8), (1, 16)), -0.2, 0.2)), 0.25, 2.5).astype(jnp.bfloat16),
    }


def reference(view_one, view_two, pair_weights):
    samples = view_one.shape[0]
    correlation = jnp.dot(view_two.T, view_one, preferred_element_type=jnp.float32) / samples
    identity = jnp.eye(D, dtype=jnp.float32)
    weighted = (pair_weights.astype(jnp.float32) * (correlation - identity)).astype(jnp.bfloat16)
    first_grad = jnp.dot(view_two, weighted, preferred_element_type=jnp.float32).astype(jnp.bfloat16)
    second_grad = jnp.dot(view_one, weighted.T, preferred_element_type=jnp.float32).astype(jnp.bfloat16)
    return first_grad, second_grad
```

```python
import functools

import jax
import jax.numpy as jnp
from jax import lax
from jax.experimental import pallas as pl
from jax.experimental.pallas import tpu as pltpu
from jax.sharding import PartitionSpec as P

ROUNDS = 2
PIECES = 2 * ROUNDS
F32 = jnp.float32
BF16 = jnp.bfloat16


def kernel(
    v1, v2, w, o1, o2,
    z1o, z1p, z2o, z2p, acc, go, gp, gr, p1, p2, rx2, rx1, rz, ry2, ry1, rzl, fin,
    lsem, ssem, k1s, k2s, zls, y1s, y2s, ts, us, x1s, x2s, gs, sx2, sx1, sz, sy2, sy1, szl, sfin,
):
    n = PIECES
    row, col = lax.axis_index("row"), lax.axis_index("col")
    y, zl = row // 2, row % 2
    x, zh, k = col // 4, (col // 2) % 2, col % 2
    samples = v1.shape[0] * v1.shape[1] * 8

    def dev(x=x, y=y, zh=zh, zl=zl, k=k):
        return (y * 2 + zl, x * 4 + zh * 2 + k)

    def mod4(a):
        return (a + 8) % 4

    xr, xl, yr, yl = mod4(x + 1), mod4(x - 1), mod4(y + 1), mod4(y - 1)
    d = mod4(x - y)
    moved = d != 0
    crossed = zh != zl
    t_dest = dev(x=mod4(x + d), y=mod4(y + d))
    t_source = dev(x=mod4(x - d), y=mod4(y - d))
    partner = dev(k=1 - k)

    started = []

    def send(src, dst, recv, where, cond=None):
        number = len(started)
        copy = pltpu.make_async_remote_copy(
            src_ref=src, dst_ref=dst, send_sem=ssem.at[number], recv_sem=recv,
            device_id=where, device_id_type=pl.DeviceIdType.MESH,
        )
        started.append((copy, cond))
        if cond is None:
            copy.start()
        else:
            pl.when(cond)(copy.start)

    def arrived(dst, recv, cond=None):
        copy = pltpu.make_async_remote_copy(
            src_ref=dst, dst_ref=dst, send_sem=ssem.at[0], recv_sem=recv,
            device_id=partner, device_id_type=pl.DeviceIdType.MESH,
        )
        if cond is None:
            copy.wait_recv()
        else:
            pl.when(cond)(copy.wait_recv)

    def slot1(yy, zz):
        return (yy * 2 + zz) * n

    def home(xx):
        return mod4(2 * y - xx)

    own = slot1(y, zl)
    load = pltpu.make_async_copy(v1, z1o.at[pl.ds(own, n)], lsem.at[0])
    load.start()
    barrier = pltpu.get_barrier_semaphore()
    for where in (
        dev(x=xr), dev(x=xl), dev(y=yr), dev(y=yl), partner,
        dev(zl=1 - zl), dev(zh=1 - zh), dev(zh=1 - zh, zl=1 - zl),
    ):
        pl.semaphore_signal(barrier, inc=1, device_id=where, device_id_type=pl.DeviceIdType.MESH)

    @pl.when(moved)
    def _():
        pl.semaphore_signal(barrier, inc=1, device_id=t_dest, device_id_type=pl.DeviceIdType.MESH)
        pl.semaphore_signal(barrier, inc=1, device_id=t_source, device_id_type=pl.DeviceIdType.MESH)

    pl.semaphore_wait(barrier, jnp.where(moved, 10, 8))

    def landing(yy):
        return jnp.where(crossed, 8 * n, slot1(yy, zl))

    first = landing(home(x))
    for piece in range(n):
        send(v2.at[piece], z2o.at[landing(y) + piece], ts.at[piece], t_dest, moved)

        @pl.when(d == 0)
        def _():
            pltpu.make_async_copy(v2.at[piece], z2o.at[first + piece], ts.at[piece]).start()

    load.wait()
    send(z1o.at[pl.ds(own, n)], z1o.at[pl.ds(own, n)], zls.at[0], dev(zl=1 - zl))
    for piece in range(n):
        send(z1o.at[own + piece], z1p.at[own + piece], k1s.at[own + piece], partner)

    def z_move(piece):
        arrived(z2o.at[first + piece], ts.at[piece], moved)

        @pl.when(d == 0)
        def _():
            pltpu.make_async_copy(v2.at[piece], z2o.at[first + piece], ts.at[piece]).wait()

        there = slot1(home(x), zl) + piece
        send(z2o.at[first + piece], z2o.at[there], us.at[zl, piece], dev(zh=1 - zl, zl=zh))
        send(z2o.at[first + piece], z2o.at[there], us.at[zl, piece], dev(zh=zl, zl=zh), crossed)

    def y_spread(zz, number):
        there = slot1(y, zz)
        block = z1o.at[pl.ds(there, n)]
        send(block, block, y1s.at[0, number], dev(y=yr))
        send(block, block, y1s.at[1, number], dev(y=yl))

    for piece in range(n):
        z_move(piece)
    y_spread(zl, 0)
    there = slot1(y, 1 - zl)
    arrived(z1o.at[pl.ds(there, n)], zls.at[0])
    y_spread(1 - zl, 1)
    for piece in range(n):
        send(z1o.at[there + piece], z1p.at[there + piece], k1s.at[there + piece], partner)

    def x_spread(zz, piece):
        there = slot1(home(x), zz) + piece
        arrived(z2o.at[there], us.at[zz, piece], jnp.logical_or(crossed, zl != zz))
        send(z2o.at[there], z2o.at[there], x1s.at[0, zz, piece], dev(x=xr))
        send(z2o.at[there], z2o.at[there], x1s.at[1, zz, piece], dev(x=xl))
        send(z2o.at[there], z2p.at[there], k2s.at[there], partner)

    for piece in range(n):
        for zz in range(2):
            x_spread(zz, piece)

    def y_forward(number):
        zz = zl if number == 0 else 1 - zl
        for side, (source, target) in enumerate(((yl, yr), (yr, yl))):
            there = slot1(source, zz)
            block = z1o.at[pl.ds(there, n)]
            arrived(block, y1s.at[side, number])
            for half in range(ROUNDS):
                piece = z1o.at[there + 2 * half + side]
                send(piece, piece, y2s.at[side, number, half], dev(y=target))
            for piece in range(n):
                send(z1o.at[there + piece], z1p.at[there + piece], k1s.at[there + piece], partner)

    def x_forward(zz, piece):
        for side, (source, target) in enumerate(((xl, xr), (xr, xl))):
            there = slot1(home(source), zz) + piece
            arrived(z2o.at[there], x1s.at[side, zz, piece])
            if piece % 2 == side:
                send(z2o.at[there], z2o.at[there], x2s.at[zz, piece], dev(x=target))
            send(z2o.at[there], z2p.at[there], k2s.at[there], partner)

    y_forward(0)
    for piece in range(n):
        if piece == n // 2:
            y_forward(1)
        for zz in range(2):
            x_forward(zz, piece)
    for number in range(2):
        zz = zl if number == 0 else 1 - zl
        there = slot1(mod4(y + 2), zz)
        for half in range(ROUNDS):
            for side in range(2):
                piece = there + 2 * half + side
                arrived(z1o.at[piece], y2s.at[side, number, half])
                send(z1o.at[piece], z1p.at[piece], k1s.at[piece], partner)

    acc[...] = jnp.zeros_like(acc)
    rows = v1.shape[0] * v1.shape[1]
    depth = v1.shape[2]
    tile = min(256, depth)

    def correlate(yy, zz):
        there = slot1(yy, zz)
        for piece in range(n):
            arrived(z2p.at[there + piece], k2s.at[there + piece])
        right = z1o[pl.ds(there, n)].reshape(rows, depth)
        for part, held in enumerate((z2o, z2p)):
            for start in range(0, depth, tile):
                left = held[pl.ds(there, n), :, pl.ds(start, tile)].reshape(rows, tile)
                acc[part, pl.ds(start, tile), :] += lax.dot_general(
                    left, right, (((0,), (0,)), ((), ())), preferred_element_type=F32
                )

    def near(step, carry):
        correlate(home(mod4(x + 3 * (step // 2 == 1) + (step // 2 == 2))), step % 2)
        return carry

    lax.fori_loop(0, 6, near, 0)
    for piece in range(n):
        for zz in range(2):
            there = slot1(home(mod4(x + 2)), zz) + piece
            arrived(z2o.at[there], x2s.at[zz, piece])
            send(z2o.at[there], z2p.at[there], k2s.at[there], partner)

    def far(step, carry):
        correlate(home(mod4(x + 2)), step)
        return carry

    lax.fori_loop(0, 2, far, 0)

    def weigh(part, target):
        half = k if part == 0 else 1 - k
        for start in range(0, depth, tile):
            shape = (tile, depth)
            row_ids = row * (2 * depth) + half * depth + start + lax.broadcasted_iota(jnp.int32, shape, 0)
            col_ids = col * depth + lax.broadcasted_iota(jnp.int32, shape, 1)
            identity = jnp.where(row_ids == col_ids, 1.0, 0.0).astype(F32)
            correlation = acc[part, pl.ds(start, tile), :] / samples
            weights = w[half, pl.ds(start, tile), :].astype(F32)
            target[pl.ds(start, tile), :] = (weights * (correlation - identity)).astype(BF16)

    weigh(1, gp)
    send(gp, gr, gs.at[0], partner)
    weigh(0, go)

    def first_part(there):
        p1[there] = (
            jnp.dot(z2o[there], go[...], preferred_element_type=F32)
            + jnp.dot(z2p[there], gp[...], preferred_element_type=F32)
        ).astype(BF16)

    turned = (((1,), (1,)), ((), ()))

    def second_part(there):
        p2[there] = (
            lax.dot_general(z1o[there], go[...], turned, preferred_element_type=F32)
            + lax.dot_general(z1p[there], gr[...], turned, preferred_element_type=F32)
        ).astype(BF16)

    def over(base, count, part):
        def body(step, carry):
            part(base(step))
            return carry

        lax.fori_loop(0, count, body, 0)

    y_far, x_far = mod4(y + 2), home(mod4(x + 2))
    over(lambda step: slot1(y_far, 0) + step, 2 * n, first_part)
    for piece in range(n):
        for zz in range(2):
            send(p1.at[slot1(y_far, zz) + piece], ry2.at[zz, piece], sy2.at[zz, piece], dev(y=yr if piece % 2 == 0 else yl))
    arrived(gr, gs.at[0])

    def all_of_z1p(step, carry):
        arrived(z1p.at[step], k1s.at[step])
        return carry

    lax.fori_loop(0, 8 * n, all_of_z1p, 0)
    over(lambda step: slot1(x_far, 0) + step, 2 * n, second_part)
    for piece in range(n):
        for zz in range(2):
            send(p2.at[slot1(x_far, zz) + piece], rx2.at[zz, piece], sx2.at[zz, piece], dev(x=xr if piece % 2 == 0 else xl))

    def around(base, here):
        def at(step):
            block = step // (2 * n)
            return base(mod4(here + (block == 0) + 3 * (block == 1))) + step % (2 * n)

        return at

    over(around(lambda xx: slot1(home(xx), 0), x), 6 * n, second_part)
    over(around(lambda yy: slot1(yy, 0), y), 6 * n, first_part)

    def pass_on(held, far_in, far_sem, near_in, near_sem, base, zz, piece, targets):
        for side, (ahead, where) in enumerate(targets):
            there = base(ahead, zz) + piece
            if piece % 2 == side:
                arrived(far_in.at[zz, piece], far_sem.at[zz, piece])
                held[there] = (held[there].astype(F32) + far_in[zz, piece].astype(F32)).astype(BF16)
            send(held.at[there], near_in.at[side, zz, piece], near_sem.at[side, zz, piece], where)

    x_targets = ((xr, dev(x=xr)), (xl, dev(x=xl)))
    y_targets = ((yr, dev(y=yr)), (yl, dev(y=yl)))
    for piece in range(n):
        for zz in range(2):
            pass_on(p2, rx2, sx2, rx1, sx1, lambda xx, zz: slot1(home(xx), zz), zz, piece, x_targets)
            pass_on(p1, ry2, sy2, ry1, sy1, slot1, zz, piece, y_targets)

    def total(held, there, near_in, near_sem, zz, piece):
        for side in range(2):
            arrived(near_in.at[side, zz, piece], near_sem.at[side, zz, piece])
        return held[there].astype(F32) + near_in[0, zz, piece].astype(F32) + near_in[1, zz, piece].astype(F32)

    for piece in range(n):
        for zz in range(2):
            there = slot1(home(x), zz) + piece
            value = total(p2, there, rx1, sx1, zz, piece).astype(BF16)
            stays = jnp.logical_and(zl == zh, zl == zz)
            p2[there] = value
            send(
                p2.at[there], rz.at[zh, piece], sz.at[zh, piece], dev(zh=zl, zl=zz), jnp.logical_not(stays)
            )

            @pl.when(stays)
            def _():
                rz[zh, piece] = value

        there = slot1(y, 0) + (1 - zl) * n + piece
        for zz in range(2):
            @pl.when(zz != zl)
            def _():
                p1[slot1(y, zz) + piece] = total(p1, slot1(y, zz) + piece, ry1, sy1, zz, piece).astype(BF16)

        send(p1.at[there], rzl.at[piece], szl.at[piece], dev(zl=1 - zl))

    for piece in range(n):
        for source in range(2):
            arrived(rz.at[source, piece], sz.at[source, piece], jnp.logical_or(crossed, zh != source))
        value = (rz[0, piece].astype(F32) + rz[1, piece].astype(F32)).astype(BF16)
        there = slot1(home(x), 0) + piece
        o2[piece] = value
        fin[0, piece] = value
        send(fin.at[0, piece], fin.at[1, piece], sfin.at[piece], t_source, moved)

    for piece in range(n):
        arrived(rzl.at[piece], szl.at[piece])
        for zz in range(2):
            @pl.when(zz == zl)
            def _():
                value = total(p1, slot1(y, zz) + piece, ry1, sy1, zz, piece)
                o1[piece] = (value + rzl[piece].astype(F32)).astype(BF16)

    for piece in range(n):
        arrived(fin.at[1, piece], sfin.at[piece], moved)

        @pl.when(moved)
        def _():
            o2[piece] = fin[1, piece]

    for copy, cond in started:
        if cond is None:
            copy.wait_send()
        else:
            pl.when(cond)(copy.wait_send)


def per_device(view_one, view_two, pair_weights):
    n = PIECES
    rows, depth = view_one.shape
    piece = (rows // n, depth)
    vmem = lambda *lead: pltpu.VMEM(lead + piece, BF16)
    square = (depth, depth)
    dma = lambda *shape: pltpu.SemaphoreType.DMA(shape)
    cut = (n,) + piece
    flops = 2 * 3 * 8 * rows * 2 * depth * depth
    first, second = pl.pallas_call(
        kernel,
        out_shape=[jax.ShapeDtypeStruct(cut, BF16)] * 2,
        in_specs=[
            pl.BlockSpec(memory_space=pltpu.HBM),
            pl.BlockSpec(memory_space=pltpu.HBM),
            pl.BlockSpec(memory_space=pltpu.VMEM),
        ],
        out_specs=[pl.BlockSpec(memory_space=pltpu.VMEM)] * 2,
        scratch_shapes=[
            vmem(8 * n), vmem(8 * n), vmem(9 * n), vmem(8 * n),
            pltpu.VMEM((2,) + square, F32),
            pltpu.VMEM(square, BF16), pltpu.VMEM(square, BF16), pltpu.VMEM(square, BF16),
            vmem(8 * n), vmem(8 * n),
            vmem(2, n), vmem(2, 2, n), vmem(2, n),
            vmem(2, n), vmem(2, 2, n), vmem(n), vmem(2, n),
            dma(1), dma(SENDS), dma(8 * n), dma(8 * n), dma(1), dma(2, 2), dma(2, 2, ROUNDS),
            dma(n), dma(2, n), dma(2, 2, n), dma(2, n), dma(1),
            dma(2, n), dma(2, 2, n), dma(2, n), dma(2, n), dma(2, 2, n), dma(n), dma(n),
        ],
        compiler_params=pltpu.CompilerParams(
            collective_id=0, has_side_effects=True, vmem_limit_bytes=60 * 1024 * 1024
        ),
        cost_estimate=pl.CostEstimate(flops=flops, bytes_accessed=8 * rows * depth, transcendentals=0),
    )(view_one.reshape(cut), view_two.reshape(cut), pair_weights.reshape((2,) + square))
    return first.reshape(rows, depth), second.reshape(rows, depth)


SENDS = 60 * PIECES


def solution(mesh):
    placed = (P("row", "col"),) * 3
    return jax.shard_map(
        per_device, mesh=mesh, in_specs=placed, out_specs=(P("row", "col"),) * 2, check_vma=False
    )
```

```python
import functools

import jax
import jax.numpy as jnp
from jax import lax
from jax.experimental import pallas as pl
from jax.experimental.pallas import tpu as pltpu
from jax.sharding import PartitionSpec as P

F32 = jnp.float32
BF16 = jnp.bfloat16
PIECES = 8
CHUNKS = 4
WIDE = PIECES // CHUNKS
LAG = 2
TURNED = (((1,), (1,)), ((), ()))


def kernel(
    v1, v2, w, o1, o2,
    z1o, z1p, z2o, z2p, acc, go, gp, gr, p1, p2, rx2, rx1, rz, ry2, ry1, rzl, fin_out, fin_in,
    lsem, ssem, k1s, k2s, zls, y1s, y2s, ts, us, x1s, x2s, gs, sx2, sx1, sz, sy2, sy1, szl, sfin,
):
    row, col = lax.axis_index("row"), lax.axis_index("col")
    y, zl = row // 2, row % 2
    x, zh, k = col // 4, (col // 2) % 2, col % 2
    depth = v1.shape[2]
    samples = v1.shape[0] * v1.shape[1] * 8
    tile = min(256, depth)

    def dev(x=x, y=y, zh=zh, zl=zl, k=k):
        return (y * 2 + zl, x * 4 + zh * 2 + k)

    def mod4(a):
        return (a + 8) % 4

    xr, xl, yr, yl = mod4(x + 1), mod4(x - 1), mod4(y + 1), mod4(y - 1)
    d = mod4(x - y)
    moved = d != 0
    crossed = zh != zl
    t_dest = dev(x=mod4(x + d), y=mod4(y + d))
    t_source = dev(x=mod4(x - d), y=mod4(y - d))
    partner = dev(k=1 - k)
    x_sides = (dev(x=xr), dev(x=xl))
    y_sides = (dev(y=yr), dev(y=yl))

    started = []

    def send(src, dst, recv, where, cond=None):
        copy = pltpu.make_async_remote_copy(
            src_ref=src, dst_ref=dst, send_sem=ssem.at[len(started)], recv_sem=recv,
            device_id=where, device_id_type=pl.DeviceIdType.MESH,
        )
        started.append((copy, cond))
        if cond is None:
            copy.start()
        else:
            pl.when(cond)(copy.start)

    def arrived(dst, recv, cond=None):
        copy = pltpu.make_async_remote_copy(
            src_ref=dst, dst_ref=dst, send_sem=ssem.at[0], recv_sem=recv,
            device_id=partner, device_id_type=pl.DeviceIdType.MESH,
        )
        if cond is None:
            copy.wait_recv()
        else:
            pl.when(cond)(copy.wait_recv)

    def home(xx):
        return mod4(2 * y - xx)

    def part(chunk):
        return pl.ds(chunk * WIDE, WIDE)

    load = pltpu.make_async_copy(v1, z1o.at[y, :, zl], lsem.at[0])
    load.start()
    barrier = pltpu.get_barrier_semaphore()
    for where in x_sides + y_sides + (
        partner, dev(zl=1 - zl), dev(zh=1 - zh), dev(zh=1 - zh, zl=1 - zl),
    ):
        pl.semaphore_signal(barrier, inc=1, device_id=where, device_id_type=pl.DeviceIdType.MESH)

    @pl.when(moved)
    def _():
        pl.semaphore_signal(barrier, inc=1, device_id=t_dest, device_id_type=pl.DeviceIdType.MESH)
        pl.semaphore_signal(barrier, inc=1, device_id=t_source, device_id_type=pl.DeviceIdType.MESH)

    pl.semaphore_wait(barrier, jnp.where(moved, 10, 8))

    spare = jnp.where(crossed, 0, zl)

    def landing(yy, chunk):
        return z2o.at[jnp.where(crossed, 4, yy), part(chunk), spare]

    def local(chunk):
        return pltpu.make_async_copy(v2.at[part(chunk)], landing(home(x), chunk), ts.at[chunk])

    for chunk in range(CHUNKS):
        send(v2.at[part(chunk)], landing(y, chunk), ts.at[chunk], t_dest, moved)
        pl.when(d == 0)(local(chunk).start)

    def share1(yy, zz, chunk):
        block = z1o.at[yy, part(chunk), zz]
        send(block, z1p.at[yy, part(chunk), zz], k1s.at[yy, zz, chunk], partner)

    def share2(yy, zz, chunk):
        block = z2o.at[yy, part(chunk), zz]
        send(block, z2p.at[yy, part(chunk), zz], k2s.at[yy, zz, chunk], partner)

    load.wait()
    send(z1o.at[y, :, zl], z1o.at[y, :, zl], zls.at[0], dev(zl=1 - zl))
    for chunk in range(CHUNKS):
        share1(y, zl, chunk)

    for chunk in range(CHUNKS):
        here = landing(home(x), chunk)
        arrived(here, ts.at[chunk], moved)
        pl.when(d == 0)(local(chunk).wait)
        there = z2o.at[home(x), part(chunk), zl]
        send(here, there, us.at[zl, chunk], dev(zh=1 - zl, zl=zh))
        send(here, there, us.at[zl, chunk], dev(zh=zl, zl=zh), crossed)

    def y_spread(number, zz):
        block = z1o.at[y, :, zz]
        for side in range(2):
            send(block, block, y1s.at[side, number], y_sides[side])

    y_spread(0, zl)
    arrived(z1o.at[y, :, 1 - zl], zls.at[0])
    y_spread(1, 1 - zl)
    for chunk in range(CHUNKS):
        share1(y, 1 - zl, chunk)

    for chunk in range(CHUNKS):
        for zz in range(2):
            block = z2o.at[home(x), part(chunk), zz]
            arrived(block, us.at[zz, chunk], jnp.logical_or(crossed, zl != zz))
            for side in range(2):
                send(block, block, x1s.at[side, zz, chunk], x_sides[side])
            share2(home(x), zz, chunk)

    def y_forward(number, zz):
        for side, source in enumerate((yl, yr)):
            arrived(z1o.at[source, :, zz], y1s.at[side, number])
            for half in range(CHUNKS // 2):
                block = z1o.at[source, part(2 * half + side), zz]
                send(block, block, y2s.at[side, number, half], y_sides[side])
            for chunk in range(CHUNKS):
                share1(source, zz, chunk)

    def x_forward(zz, chunk):
        for side, source in enumerate((xl, xr)):
            block = z2o.at[home(source), part(chunk), zz]
            arrived(block, x1s.at[side, zz, chunk])
            if chunk % 2 == side:
                send(block, block, x2s.at[zz, chunk], x_sides[side])
            share2(home(source), zz, chunk)

    y_forward(0, zl)
    for chunk in range(CHUNKS):
        if chunk == CHUNKS // 2:
            y_forward(1, 1 - zl)
        for zz in range(2):
            x_forward(zz, chunk)

    def flat(ref, yy, columns=slice(None)):
        block = ref[yy, :, :, :, columns]
        return block.reshape(-1, block.shape[-1])

    def correlate(yy):
        for zz in range(2):
            for chunk in range(CHUNKS):
                arrived(z2p.at[yy, part(chunk), zz], k2s.at[yy, zz, chunk])
        right = flat(z1o, yy)
        for number, held in enumerate((z2o, z2p)):
            for start in range(0, depth, tile):
                left = flat(held, yy, pl.ds(start, tile))
                acc[number, pl.ds(start, tile), :] += lax.dot_general(
                    left, right, (((0,), (0,)), ((), ())), preferred_element_type=F32
                )

    def early(step, carry):
        first = jnp.where(d == 2, 1, 0)
        second = jnp.where(jnp.logical_or(d == 0, d == 3), 1, 3)
        correlate(home(mod4(x + jnp.where(step == 0, first, second))))
        return carry

    acc[...] = jnp.zeros_like(acc)
    lax.fori_loop(0, 2, early, 0)
    for number in range(2):
        zz = zl if number == 0 else 1 - zl
        for half in range(CHUNKS // 2):
            for side in range(2):
                chunk = 2 * half + side
                arrived(z1o.at[mod4(y + 2), part(chunk), zz], y2s.at[side, number, half])
                share1(mod4(y + 2), zz, chunk)
    for chunk in range(CHUNKS):
        for zz in range(2):
            arrived(z2o.at[home(mod4(x + 2)), part(chunk), zz], x2s.at[zz, chunk])
            share2(home(mod4(x + 2)), zz, chunk)

    def late(step, carry):
        correlate(home(mod4(x + jnp.where(step == 0, jnp.where(d == 0, 3, 2 - d), 2))))
        return carry

    lax.fori_loop(0, 2, late, 0)

    def weigh(number, target):
        half = k if number == 0 else 1 - k
        for start in range(0, depth, tile):
            shape = (tile, depth)
            row_ids = row * (2 * depth) + half * depth + start + lax.broadcasted_iota(jnp.int32, shape, 0)
            col_ids = col * depth + lax.broadcasted_iota(jnp.int32, shape, 1)
            identity = jnp.where(row_ids == col_ids, 1.0, 0.0).astype(F32)
            correlation = acc[number, pl.ds(start, tile), :] / samples
            weights = w[half, pl.ds(start, tile), :].astype(F32)
            target[pl.ds(start, tile), :] = (weights * (correlation - identity)).astype(BF16)

    weigh(1, gp)
    send(gp, gr, gs.at[0], partner)
    weigh(0, go)

    size = PIECES // 2

    def slab(ref, yy, s):
        return ref[yy, pl.ds(s * size, size)].reshape(-1, depth)

    def first_part(yy, s):
        total = jnp.dot(slab(z2o, yy, s), go[...], preferred_element_type=F32)
        total += jnp.dot(slab(z2p, yy, s), gp[...], preferred_element_type=F32)
        p1[yy, pl.ds(s * size, size)] = total.astype(BF16).reshape((size,) + p1.shape[2:])

    def second_part(yy, s):
        total = lax.dot_general(slab(z1o, yy, s), go[...], TURNED, preferred_element_type=F32)
        total += lax.dot_general(slab(z1p, yy, s), gr[...], TURNED, preferred_element_type=F32)
        p2[yy, pl.ds(s * size, size)] = total.astype(BF16).reshape((size,) + p2.shape[2:])

    def pieces(s):
        return range(s * size, (s + 1) * size)

    def to_far(held, yy, s, far_in, far_sem, sides):
        for p in pieces(s):
            send(held.at[yy, p], far_in.at[p], far_sem.at[p], sides[p % 2])

    y_far, x_far = mod4(y + 2), home(mod4(x + 2))
    first_part(y_far, 0)
    to_far(p1, y_far, 0, ry2, sy2, y_sides)
    arrived(gr, gs.at[0])

    def all_of_z1p(step, carry):
        for zz in range(2):
            for chunk in range(CHUNKS):
                arrived(z1p.at[step, part(chunk), zz], k1s.at[step, zz, chunk])
        return carry

    lax.fori_loop(0, 4, all_of_z1p, 0)
    for s in range(2):
        second_part(x_far, s)
        to_far(p2, x_far, s, rx2, sx2, x_sides)
    first_part(y_far, 1)
    to_far(p1, y_far, 1, ry2, sy2, y_sides)

    def to_near(held, ahead, s, far_in, far_sem, near_in, near_sem, sides):
        for p in pieces(s):
            side = 1 - p % 2
            send(held.at[ahead[side], p], near_in.at[side, p], near_sem.at[side, p], sides[side])

    def to_near_with(held, ahead, s, far_in, far_sem, near_in, near_sem, sides):
        for p in pieces(s):
            side = p % 2
            arrived(far_in.at[p], far_sem.at[p])
            yy = ahead[side]
            held[yy, p] = (held[yy, p].astype(F32) + far_in[p].astype(F32)).astype(BF16)
            send(held.at[yy, p], near_in.at[side, p], near_sem.at[side, p], sides[side])

    for s in range(2):
        def near_x(step, carry):
            second_part(home(mod4(x + 1 + 2 * step)), s)
            return carry

        def near_y(step, carry):
            first_part(mod4(y + 1 + 2 * step), s)
            return carry

        along_x = (p2, (home(xr), home(xl)), s, rx2, sx2, rx1, sx1, x_sides)
        along_y = (p1, (yr, yl), s, ry2, sy2, ry1, sy1, y_sides)
        lax.fori_loop(0, 2, near_x, 0)
        to_near(*along_x)
        lax.fori_loop(0, 2, near_y, 0)
        to_near(*along_y)
        to_near_with(*along_x)
        to_near_with(*along_y)

    def own(step, carry):
        second_part(home(x), step)
        first_part(y, step)
        return carry

    lax.fori_loop(0, 2, own, 0)

    for p in range(PIECES + LAG):
        if p < PIECES:
            for side in range(2):
                arrived(rx1.at[side, p], sx1.at[side, p])
            value = p2[home(x), p].astype(F32) + rx1[0, p].astype(F32) + rx1[1, p].astype(F32)
            p2[home(x), p] = value.astype(BF16)
            for zz in range(2):
                stays = jnp.logical_and(zl == zh, zl == zz)
                send(
                    p2.at[home(x), p, zz], rz.at[zh, p], sz.at[zh, p], dev(zh=zl, zl=zz), jnp.logical_not(stays)
                )

                @pl.when(stays)
                def _():
                    rz[zh, p] = p2[home(x), p, zz]

            for side in range(2):
                arrived(ry1.at[side, p], sy1.at[side, p])

            def of_y(zz):
                return (
                    p1[y, p, zz].astype(F32) + ry1[0, p, zz].astype(F32) + ry1[1, p, zz].astype(F32)
                )

            p1[y, p, 1 - zl] = of_y(1 - zl).astype(BF16)
            send(p1.at[y, p, 1 - zl], rzl.at[p], szl.at[p], dev(zl=1 - zl))
        if p >= LAG:
            q = p - LAG
            for source in range(2):
                arrived(rz.at[source, q], sz.at[source, q], jnp.logical_or(crossed, zh != source))
            value = (rz[0, q].astype(F32) + rz[1, q].astype(F32)).astype(BF16)
            o2[q] = value
            fin_out[q] = value
            send(fin_out.at[q], fin_in.at[q], sfin.at[q], t_source, moved)
            arrived(rzl.at[q], szl.at[q])
            value = p1[y, q, zl].astype(F32) + ry1[0, q, zl].astype(F32) + ry1[1, q, zl].astype(F32)
            o1[q] = (value + rzl[q].astype(F32)).astype(BF16)

    for p in range(PIECES):
        arrived(fin_in.at[p], sfin.at[p], moved)

        @pl.when(moved)
        def _():
            o2[p] = fin_in[p]

    for copy, cond in started:
        if cond is None:
            copy.wait_send()
        else:
            pl.when(cond)(copy.wait_send)


SENDS = 320


def per_device(view_one, view_two, pair_weights):
    n = PIECES
    rows, depth = view_one.shape
    piece = (rows // n, depth)
    vmem = lambda *lead: pltpu.VMEM(lead + piece, BF16)
    square = (depth, depth)
    dma = lambda *shape: pltpu.SemaphoreType.DMA(shape)
    cut = (n,) + piece
    flops = 2 * 3 * 8 * rows * 2 * depth * depth
    first, second = pl.pallas_call(
        kernel,
        out_shape=[jax.ShapeDtypeStruct(cut, BF16)] * 2,
        in_specs=[
            pl.BlockSpec(memory_space=pltpu.HBM),
            pl.BlockSpec(memory_space=pltpu.HBM),
            pl.BlockSpec(memory_space=pltpu.VMEM),
        ],
        out_specs=[pl.BlockSpec(memory_space=pltpu.VMEM)] * 2,
        scratch_shapes=[
            vmem(4, n, 2), vmem(4, n, 2), vmem(5, n, 2), vmem(4, n, 2),
            pltpu.VMEM((2,) + square, F32),
            pltpu.VMEM(square, BF16), pltpu.VMEM(square, BF16), pltpu.VMEM(square, BF16),
            vmem(4, n, 2), vmem(4, n, 2),
            vmem(n, 2), vmem(2, n, 2), vmem(2, n),
            vmem(n, 2), vmem(2, n, 2), vmem(n), vmem(n), vmem(n),
            dma(1), dma(SENDS), dma(4, 2, CHUNKS), dma(4, 2, CHUNKS), dma(1), dma(2, 2), dma(2, 2, CHUNKS // 2),
            dma(CHUNKS), dma(2, CHUNKS), dma(2, 2, CHUNKS), dma(2, CHUNKS), dma(1),
            dma(n), dma(2, n), dma(2, n), dma(n), dma(2, n), dma(n), dma(n),
        ],
        compiler_params=pltpu.CompilerParams(
            collective_id=0, has_side_effects=True, vmem_limit_bytes=60 * 1024 * 1024
        ),
        cost_estimate=pl.CostEstimate(flops=flops, bytes_accessed=8 * rows * depth, transcendentals=0),
    )(view_one.reshape(cut), view_two.reshape(cut), pair_weights.reshape((2,) + square))
    return first.reshape(rows, depth), second.reshape(rows, depth)


def solution(mesh):
    placed = (P("row", "col"),) * 3
    return jax.shard_map(
        per_device, mesh=mesh, in_specs=placed, out_specs=(P("row", "col"),) * 2, check_vma=False
    )
```

```python
import functools

import jax
import jax.numpy as jnp
from jax import lax
from jax.experimental import pallas as pl
from jax.experimental.pallas import tpu as pltpu
from jax.sharding import PartitionSpec as P

F32 = jnp.float32
BF16 = jnp.bfloat16
PIECES = 8
CHUNKS = 4
WIDE = PIECES // CHUNKS
LAG = 2
YLAG = 1
SEQUENCE = tuple(range(PIECES))
TURNED = (((1,), (1,)), ((), ()))


def kernel(
    v1, v2, w_hbm, o1, o2,
    w, z1o, z1p, z2o, z2p, acc, go, gp, gr, p1, p2, rx2, rx1, rz, ry2, ry1, rzl, fin_out, fin_in,
    lsem, ssem, k1s, k2s, zls, y1s, y2s, ts, rs, us, x1s, x2s, gs, sx2, sx1, sz, sy2, sy1, szl, sfin,
):
    row, col = lax.axis_index("row"), lax.axis_index("col")
    y, zl = row // 2, row % 2
    x, zh, k = col // 4, (col // 2) % 2, col % 2
    depth = v1.shape[2]
    samples = v1.shape[0] * v1.shape[1] * 8
    tile = min(256, depth)

    def dev(x=x, y=y, zh=zh, zl=zl, k=k):
        return (y * 2 + zl, x * 4 + zh * 2 + k)

    def mod4(a):
        return (a + 8) % 4

    xr, xl, yr, yl = mod4(x + 1), mod4(x - 1), mod4(y + 1), mod4(y - 1)
    d = mod4(x - y)
    moved = d != 0
    crossed = zh != zl
    straight = zh == zl
    partner = dev(k=1 - k)
    x_sides = (dev(x=xr), dev(x=xl))
    y_sides = (dev(y=yr), dev(y=yl))

    groups = []

    def send(src, dst, recv, where, cond=None):
        size = 1
        for extent in src.shape[:-2]:
            size *= extent
        if len(src.shape) == 2 and src.shape != v1.shape[1:]:
            size = GROUP
        for group in groups:
            if group[0] == size and group[1] is cond and group[2] + size <= GROUP:
                break
        else:
            group = [size, cond, 0, len(groups)]
            groups.append(group)
        group[2] += size
        copy = pltpu.make_async_remote_copy(
            src_ref=src, dst_ref=dst, send_sem=ssem.at[group[3]], recv_sem=recv,
            device_id=where, device_id_type=pl.DeviceIdType.MESH,
        )
        if cond is None:
            copy.start()
        else:
            pl.when(cond)(copy.start)

    def arrived(dst, recv, cond=None):
        copy = pltpu.make_async_remote_copy(
            src_ref=dst, dst_ref=dst, send_sem=ssem.at[0], recv_sem=recv,
            device_id=partner, device_id_type=pl.DeviceIdType.MESH,
        )
        if cond is None:
            copy.wait_recv()
        else:
            pl.when(cond)(copy.wait_recv)

    def home(xx, half):
        return mod4(2 * y - xx + (2 * (xx % 2) - 1) * half)

    t_dest = [dev(x=mod4(x + d + (1 - 2 * (y % 2)) * half), y=x) for half in range(2)]
    t_source = [dev(x=y, y=home(x, half)) for half in range(2)]

    def part(chunk):
        return pl.ds(chunk * WIDE, WIDE)

    load = pltpu.make_async_copy(v1, z1o.at[y, :, zl], lsem.at[0])
    load.start()
    fetch = pltpu.make_async_copy(w_hbm, w, lsem.at[1])
    fetch.start()
    barrier = pltpu.get_barrier_semaphore()
    for where in x_sides + y_sides + (
        partner, dev(zl=1 - zl), dev(zh=1 - zh), dev(zh=1 - zh, zl=1 - zl),
        t_dest[1], t_source[1],
    ):
        pl.semaphore_signal(barrier, inc=1, device_id=where, device_id_type=pl.DeviceIdType.MESH)

    @pl.when(moved)
    def _():
        pl.semaphore_signal(barrier, inc=1, device_id=t_dest[0], device_id_type=pl.DeviceIdType.MESH)
        pl.semaphore_signal(barrier, inc=1, device_id=t_source[0], device_id_type=pl.DeviceIdType.MESH)

    pl.semaphore_wait(barrier, jnp.where(moved, 12, 10))

    spare = jnp.where(crossed, 0, zl)

    def landing(yy, chunk):
        return z2o.at[jnp.where(crossed, 4, yy), part(chunk), spare]

    def local(chunk):
        return pltpu.make_async_copy(v2.at[part(chunk)], landing(home(x, 0), chunk), ts.at[chunk])

    order = (0, 2, 1, 3)
    for chunk in order:
        half = chunk // 2
        send(v2.at[part(chunk)], landing(y, chunk), ts.at[chunk], t_dest[half], None if half else moved)
        if half == 0:
            pl.when(d == 0)(local(chunk).start)

    def share1(yy, zz, chunk):
        block = z1o.at[yy, part(chunk), zz]
        send(block, z1p.at[yy, part(chunk), zz], k1s.at[0], partner)

    def share2(xx, zz, chunk, cond=None):
        block = held2(xx, zz, chunk)
        send(block, z2p.at[home(xx, chunk // 2), part(chunk), zz], k2s.at[home(xx, chunk // 2), chunk // 2], partner, cond)

    def held2(xx, zz, chunk):
        return z2o.at[home(xx, chunk // 2), part(chunk), zz]

    load.wait()

    def y_spread(number, zz, chunk):
        block = z1o.at[y, part(chunk), zz]
        for side in range(2):
            send(block, block, y1s.at[side, number, chunk], y_sides[side])

    def zl_swap(chunk):
        block = z1o.at[y, part(chunk), zl]
        send(block, block, zls.at[chunk], dev(zl=1 - zl))

    def x_spread(zz, chunk, cond):
        block = held2(x, zz, chunk)
        for side in range(2):
            send(block, block, x1s.at[side, zz, chunk], x_sides[side], cond)
        share2(x, zz, chunk, cond)

    def z_move(chunk):
        here = landing(home(x, chunk // 2), chunk)
        if chunk // 2:
            arrived(here, ts.at[chunk])
        else:
            arrived(here, ts.at[chunk], moved)
            pl.when(d == 0)(local(chunk).wait)
        there = held2(x, zl, chunk)
        for target in (dev(zh=1 - zl, zl=zh), dev(zh=zl, zl=zh)):
            send(here, there, us.at[zl, chunk], target, crossed)
        send(here, z2o.at[4, part(chunk), 0], rs.at[chunk], dev(zh=1 - zh, zl=1 - zl), straight)
        x_spread(zl, chunk, straight)

    def relay(chunk):
        here = z2o.at[4, part(chunk), 0]
        arrived(here, rs.at[chunk], straight)
        send(here, held2(x, 1 - zl, chunk), us.at[1 - zl, chunk], dev(zl=1 - zl), straight)

    def x_direct(chunk):
        arrived(held2(x, 1 - zl, chunk), us.at[1 - zl, chunk])
        x_spread(1 - zl, chunk, None)

    def x_relayed(chunk):
        arrived(held2(x, zl, chunk), us.at[zl, chunk], crossed)
        x_spread(zl, chunk, crossed)

    def y_forward(number, chunk):
        zz = zl if number == 0 else 1 - zl
        for side, source in enumerate((yl, yr)):
            block = z1o.at[source, part(chunk), zz]
            arrived(block, y1s.at[side, number, chunk])
            if chunk % 2 == side:
                send(block, block, y2s.at[number, chunk], y_sides[side])
            share1(source, zz, chunk)

    def x_forward(chunk):
        for zz in range(2):
            for side, source in enumerate((xl, xr)):
                block = held2(source, zz, chunk)
                arrived(block, x1s.at[side, zz, chunk])
                if chunk % 2 == side:
                    send(block, block, x2s.at[zz, chunk], x_sides[side])
                share2(source, zz, chunk)

    def zl_step(chunk):
        arrived(z1o.at[y, part(chunk), 1 - zl], zls.at[chunk])
        y_spread(1, 1 - zl, chunk)
        share1(y, 1 - zl, chunk)

    a, b, c, e = order
    zl_swap(a)
    for chunk in order:
        y_spread(0, zl, chunk)
    for chunk in order:
        z_move(chunk)
    zl_swap(b)
    zl_step(a)
    for chunk in order:
        share1(y, zl, chunk)
    x_direct(a)
    relay(a)
    x_direct(b)
    relay(b)
    zl_swap(c)
    x_direct(c)
    relay(c)
    x_relayed(a)
    zl_swap(e)
    x_direct(e)
    relay(e)
    x_relayed(b)
    y_forward(0, a)
    y_forward(0, b)
    zl_step(b)
    x_relayed(c)
    y_forward(0, c)
    y_forward(0, e)
    zl_step(c)
    x_relayed(e)
    x_forward(a)
    zl_step(e)
    y_forward(1, a)
    x_forward(b)
    y_forward(1, b)
    x_forward(c)
    y_forward(1, c)
    x_forward(e)
    y_forward(1, e)

    size = PIECES // 2

    def slab(ref, yy, s, columns=slice(None)):
        block = ref[yy, pl.ds(s * size, size), :, :, columns]
        return block.reshape(-1, block.shape[-1])

    def correlate(yy, s):
        arrived(z2p.at[yy, pl.ds(s * size, size)], k2s.at[yy, s])
        right = slab(z1o, yy, s)
        for number, held in enumerate((z2o, z2p)):
            for start in range(0, depth, tile):
                left = slab(held, yy, s, pl.ds(start, tile))
                acc[number, pl.ds(start, tile), :] += lax.dot_general(
                    left, right, (((0,), (0,)), ((), ())), preferred_element_type=F32
                )

    def last_along_y(half):
        return mod4(2 - d + (1 - 2 * (y % 2)) * half)

    def early(step, carry):
        half = step % 2
        late_one = last_along_y(half)
        first = jnp.where(late_one == 0, 1, 0)
        second = jnp.where(late_one < 2, 3, 1)
        correlate(home(mod4(x + jnp.where(step < 2, first, second)), half), half)
        return carry

    acc[...] = jnp.zeros_like(acc)
    lax.fori_loop(0, 4, early, 0)
    for number in range(2):
        zz = zl if number == 0 else 1 - zl
        for chunk in range(CHUNKS):
            arrived(z1o.at[mod4(y + 2), part(chunk), zz], y2s.at[number, chunk])
            share1(mod4(y + 2), zz, chunk)

    def third(step, carry):
        late_one = last_along_y(step)
        correlate(home(mod4(x + jnp.where(late_one == 2, 3, late_one)), step), step)
        return carry

    lax.fori_loop(0, 2, third, 0)
    for chunk in order:
        for zz in range(2):
            arrived(held2(mod4(x + 2), zz, chunk), x2s.at[zz, chunk])
            share2(mod4(x + 2), zz, chunk)

    def last(step, carry):
        correlate(home(mod4(x + 2), step), step)
        return carry

    lax.fori_loop(0, 2, last, 0)

    def weigh(number, target):
        half = k if number == 0 else 1 - k
        for start in range(0, depth, tile):
            shape = (tile, depth)
            row_ids = row * (2 * depth) + half * depth + start + lax.broadcasted_iota(jnp.int32, shape, 0)
            col_ids = col * depth + lax.broadcasted_iota(jnp.int32, shape, 1)
            identity = jnp.where(row_ids == col_ids, 1.0, 0.0).astype(F32)
            correlation = acc[number, pl.ds(start, tile), :] / samples
            weights = w[half, pl.ds(start, tile), :].astype(F32)
            target[pl.ds(start, tile), :] = (weights * (correlation - identity)).astype(BF16)

    fetch.wait()
    weigh(1, gp)
    send(gp, gr, gs.at[0], partner)
    weigh(0, go)
    arrived(z1p, k1s.at[0])

    def first_part(yy, s):
        total = jnp.dot(slab(z2o, yy, s), go[...], preferred_element_type=F32)
        total += jnp.dot(slab(z2p, yy, s), gp[...], preferred_element_type=F32)
        p1[yy, pl.ds(s * size, size)] = total.astype(BF16).reshape((size,) + p1.shape[2:])

    def second_part(yy, s, ready=None):
        total = lax.dot_general(slab(z1o, yy, s), go[...], TURNED, preferred_element_type=F32)
        if ready is not None:
            ready()
        total += lax.dot_general(slab(z1p, yy, s), gr[...], TURNED, preferred_element_type=F32)
        p2[yy, pl.ds(s * size, size)] = total.astype(BF16).reshape((size,) + p2.shape[2:])

    def pieces(s):
        return range(s * size, (s + 1) * size)

    def to_far(held, yy, s, far_in, far_sem, sides):
        for p in pieces(s):
            send(held.at[yy, p], far_in.at[p], far_sem.at[p], sides[p % 2])

    def far_x(s, ready=None):
        second_part(home(mod4(x + 2), s), s, ready)
        to_far(p2, home(mod4(x + 2), s), s, rx2, sx2, x_sides)

    def far_y(s):
        first_part(mod4(y + 2), s)
        to_far(p1, mod4(y + 2), s, ry2, sy2, y_sides)

    far_y(0)
    far_x(0, lambda: arrived(gr, gs.at[0]))
    far_x(1)
    far_y(1)

    def to_near(held, ahead, p, far_in, far_sem, near_in, near_sem, sides, which=(0, 1)):
        for side in which:
            yy = ahead[side]
            if p % 2 == side:
                arrived(far_in.at[p], far_sem.at[p])
                held[yy, p] = (held[yy, p].astype(F32) + far_in[p].astype(F32)).astype(BF16)
            send(held.at[yy, p], near_in.at[side, p], near_sem.at[side, p], sides[side])

    def along_x(p, which=(0, 1)):
        to_near(p2, (home(xr, p // size), home(xl, p // size)), p, rx2, sx2, rx1, sx1, x_sides, which)

    def along_y(p, which=(0, 1)):
        to_near(p1, (yr, yl), p, ry2, sy2, ry1, sy1, y_sides, which)

    for s in range(2):
        def near_x(step, carry):
            second_part(home(mod4(x + 1 + 2 * step), s), s)
            return carry

        def near_y(step, carry):
            first_part(mod4(y + 1 + 2 * step), s)
            return carry

        lax.fori_loop(0, 2, near_x, 0)
        for p in range(s * size, (s + 1) * size):
            along_x(p)
        lax.fori_loop(0, 2, near_y, 0)
        for p in range(s * size, (s + 1) * size):
            along_y(p)

    def own(step, carry):
        second_part(home(x, step), step)
        first_part(y, step)
        return carry

    lax.fori_loop(0, 2, own, 0)

    goes = [jnp.logical_or(crossed, zl != zz) for zz in range(2)]

    def x_total(p):
        here = home(x, p // size)
        for side in range(2):
            arrived(rx1.at[side, p], sx1.at[side, p])
        value = p2[here, p].astype(F32) + rx1[0, p].astype(F32) + rx1[1, p].astype(F32)
        p2[here, p] = value.astype(BF16)
        for zz in range(2):
            send(p2.at[here, p, zz], rz.at[zh, p], sz.at[zh, p], dev(zh=zl, zl=zz), goes[zz])

            @pl.when(jnp.logical_not(goes[zz]))
            def _():
                rz[zh, p] = p2[here, p, zz]

    def x_final(p):
        for source in range(2):
            arrived(rz.at[source, p], sz.at[source, p], jnp.logical_or(crossed, zh != source))
        value = (rz[0, p].astype(F32) + rz[1, p].astype(F32)).astype(BF16)
        fin_out[p] = value
        if p < size:
            o2[p] = value
            send(fin_out.at[p], fin_in.at[p], sfin.at[p], t_source[0], moved)
        else:
            send(fin_out.at[p], fin_in.at[p], sfin.at[p], t_source[1])

    def of_y(p, zz):
        return p1[y, p, zz].astype(F32) + ry1[0, p, zz].astype(F32) + ry1[1, p, zz].astype(F32)

    def y_total(p):
        for side in range(2):
            arrived(ry1.at[side, p], sy1.at[side, p])
        p1[y, p, 1 - zl] = of_y(p, 1 - zl).astype(BF16)
        send(p1.at[y, p, 1 - zl], rzl.at[p], szl.at[p], dev(zl=1 - zl))

    def y_final(p):
        arrived(rzl.at[p], szl.at[p])
        o1[p] = (of_y(p, zl) + rzl[p].astype(F32)).astype(BF16)

    for turn in range(PIECES + LAG + YLAG):
        for lag, stage in ((0, x_total), (LAG, x_final), (YLAG, y_total), (LAG + YLAG, y_final)):
            if 0 <= turn - lag < PIECES:
                stage(SEQUENCE[turn - lag])

    for p in SEQUENCE:
        if p < size:
            arrived(fin_in.at[p], sfin.at[p], moved)

            @pl.when(moved)
            def _():
                o2[p] = fin_in[p]
        else:
            arrived(fin_in.at[p], sfin.at[p])
            o2[p] = fin_in[p]

    for size, cond, pieces_sent, number in groups:
        if size == GROUP:
            ref = gp
        elif pieces_sent % 2:
            ref = z1p.at[0, pl.ds(0, pieces_sent), 0]
        else:
            ref = z1p.at[0, pl.ds(0, pieces_sent // 2)]
        copy = pltpu.make_async_remote_copy(
            src_ref=ref, dst_ref=ref, send_sem=ssem.at[number], recv_sem=ssem.at[number],
            device_id=partner, device_id_type=pl.DeviceIdType.MESH,
        )
        if cond is None:
            copy.wait_send()
        else:
            pl.when(cond)(copy.wait_send)


GROUP = 2 * PIECES
SENDS = 56


def per_device(view_one, view_two, pair_weights):
    n = PIECES
    rows, depth = view_one.shape
    piece = (rows // n, depth)
    vmem = lambda *lead: pltpu.VMEM(lead + piece, BF16)
    square = (depth, depth)
    dma = lambda *shape: pltpu.SemaphoreType.DMA(shape)
    cut = (n,) + piece
    flops = 2 * 3 * 8 * rows * 2 * depth * depth
    first, second = pl.pallas_call(
        kernel,
        out_shape=[jax.ShapeDtypeStruct(cut, BF16)] * 2,
        in_specs=[
            pl.BlockSpec(memory_space=pltpu.HBM),
            pl.BlockSpec(memory_space=pltpu.HBM),
            pl.BlockSpec(memory_space=pltpu.HBM),
        ],
        out_specs=[pl.BlockSpec(memory_space=pltpu.VMEM)] * 2,
        scratch_shapes=[
            pltpu.VMEM((2,) + square, BF16),
            vmem(4, n, 2), vmem(4, n, 2), vmem(5, n, 2), vmem(4, n, 2),
            pltpu.VMEM((2,) + square, F32),
            pltpu.VMEM(square, BF16), pltpu.VMEM(square, BF16), pltpu.VMEM(square, BF16),
            vmem(4, n, 2), vmem(4, n, 2),
            vmem(n, 2), vmem(2, n, 2), vmem(2, n),
            vmem(n, 2), vmem(2, n, 2), vmem(n), vmem(n), vmem(n),
            dma(2), dma(SENDS), dma(1), dma(4, 2), dma(CHUNKS), dma(2, 2, CHUNKS), dma(2, CHUNKS),
            dma(CHUNKS), dma(CHUNKS), dma(2, CHUNKS), dma(2, 2, CHUNKS), dma(2, CHUNKS), dma(1),
            dma(n), dma(2, n), dma(2, n), dma(n), dma(2, n), dma(n), dma(n),
        ],
        compiler_params=pltpu.CompilerParams(
            collective_id=0, has_side_effects=True, vmem_limit_bytes=60 * 1024 * 1024
        ),
        cost_estimate=pl.CostEstimate(flops=flops, bytes_accessed=8 * rows * depth, transcendentals=0),
    )(view_one.reshape(cut), view_two.reshape(cut), pair_weights.reshape((2,) + square))
    return first.reshape(rows, depth), second.reshape(rows, depth)


def solution(mesh):
    placed = (P("row", "col"),) * 3
    return jax.shard_map(
        per_device, mesh=mesh, in_specs=placed, out_specs=(P("row", "col"),) * 2, check_vma=False
    )
```

```python
import functools

import jax
import jax.numpy as jnp
from jax import lax
from jax.experimental import pallas as pl
from jax.experimental.pallas import tpu as pltpu
from jax.sharding import PartitionSpec as P

F32 = jnp.float32
BF16 = jnp.bfloat16
PIECES = 8
CHUNKS = 4
WIDE = PIECES // CHUNKS
LAG = 2
AHEAD = 3
ONWARD = 5
Y_LAG = 4
TURNED = (((1,), (1,)), ((), ()))


def kernel(
    v1, v2, w_hbm, o1, o2,
    w, z1o, z1p, z2o, z2p, acc, go, gp, gr, p1, p2, rx2, rx1, rz, ry2, ry1, rzl, fin_out, mid, fin_in, tally,
    lsem, ssem, k1s, k2s, zls, y1s, y2s, ts, rs, us, x1s, x2s, gs, sx2, sx1, sz, sy2, sy1, szl, smid, sfin,
):
    row, col = lax.axis_index("row"), lax.axis_index("col")
    y, zl = row // 2, row % 2
    x, zh, k = col // 4, (col // 2) % 2, col % 2
    depth = v1.shape[2]
    samples = v1.shape[0] * v1.shape[1] * 8
    tile = min(256, depth)

    def dev(x=x, y=y, zh=zh, zl=zl, k=k):
        return (y * 2 + zl, x * 4 + zh * 2 + k)

    def mod4(a):
        return (a + 8) % 4

    xr, xl, yr, yl = mod4(x + 1), mod4(x - 1), mod4(y + 1), mod4(y - 1)
    crossed = zh != zl
    straight = zh == zl
    partner = dev(k=1 - k)
    x_sides = (dev(x=xr), dev(x=xl))
    y_sides = (dev(y=yr), dev(y=yl))

    groups = []

    def send(src, dst, recv, where, cond=None):
        size = 1
        for extent in src.shape[:-2]:
            size *= extent
        if len(src.shape) == 2 and src.shape != v1.shape[1:]:
            size = GROUP
        for group in groups:
            if group[0] == size and group[1] is cond and group[2] + size <= GROUP:
                break
        else:
            group = [size, cond, 0, len(groups)]
            groups.append(group)
        group[2] += size
        copy = pltpu.make_async_remote_copy(
            src_ref=src, dst_ref=dst, send_sem=ssem.at[group[3]], recv_sem=recv,
            device_id=where, device_id_type=pl.DeviceIdType.MESH,
        )
        if cond is None:
            copy.start()
        else:
            pl.when(cond)(copy.start)

    def arrived(dst, recv, cond=None):
        copy = pltpu.make_async_remote_copy(
            src_ref=dst, dst_ref=dst, send_sem=ssem.at[0], recv_sem=recv,
            device_id=partner, device_id_type=pl.DeviceIdType.MESH,
        )
        if cond is None:
            copy.wait_recv()
        else:
            pl.when(cond)(copy.wait_recv)

    def home(xx, half):
        return mod4(y - xx + 2 * half)

    t_dest = [dev(x=mod4(x - y + 2 * half), y=x) for half in range(2)]
    t_source = [dev(x=y, y=home(x, half)) for half in range(2)]
    moves_y = [x != 2 * half for half in range(2)]
    moves_x = [y != 2 * half for half in range(2)]
    moved = [jnp.logical_or(moves_x[half], moves_y[half]) for half in range(2)]

    def part(chunk):
        return pl.ds(chunk * WIDE, WIDE)

    load = pltpu.make_async_copy(v1, z1o.at[y, :, zl], lsem.at[0])
    load.start()
    fetch = pltpu.make_async_copy(w_hbm, w, lsem.at[1])
    fetch.start()
    barrier = pltpu.get_barrier_semaphore()
    for where in x_sides + y_sides + (
        partner, dev(zl=1 - zl), dev(zh=1 - zh), dev(zh=1 - zh, zl=1 - zl), dev(x=mod4(x + 2)), dev(y=mod4(y + 2)),
    ):
        pl.semaphore_signal(barrier, inc=1, device_id=where, device_id_type=pl.DeviceIdType.MESH)
    for half in range(2):
        @pl.when(moved[half])
        def _():
            for where in (t_dest[half], t_source[half]):
                pl.semaphore_signal(barrier, inc=1, device_id=where, device_id_type=pl.DeviceIdType.MESH)

    own_blocks = jnp.logical_and(x == y, x % 2 == 0)
    pl.semaphore_wait(barrier, jnp.where(own_blocks, 12, 14))

    spare = jnp.where(crossed, 0, zl)

    def landing(yy, chunk):
        return z2o.at[jnp.where(crossed, 4, yy), part(chunk), spare]

    def local(chunk):
        return pltpu.make_async_copy(v2.at[part(chunk)], landing(home(x, chunk // 2), chunk), ts.at[chunk])

    order = (0, 2, 1, 3)
    for chunk in order:
        half = chunk // 2
        send(v2.at[part(chunk)], landing(y, chunk), ts.at[chunk], t_dest[half], moved[half])
        pl.when(jnp.logical_not(moved[half]))(local(chunk).start)

    def share1(yy, zz, chunk):
        block = z1o.at[yy, part(chunk), zz]
        send(block, z1p.at[yy, part(chunk), zz], k1s.at[0], partner)

    def share2(xx, zz, chunk, cond=None):
        block = held2(xx, zz, chunk)
        send(block, z2p.at[home(xx, chunk // 2), part(chunk), zz], k2s.at[home(xx, chunk // 2), chunk // 2], partner, cond)

    def held2(xx, zz, chunk):
        return z2o.at[home(xx, chunk // 2), part(chunk), zz]

    load.wait()

    def y_spread(number, zz, chunk):
        block = z1o.at[y, part(chunk), zz]
        for side in range(2):
            send(block, block, y1s.at[side, number, chunk], y_sides[side])

    def zl_swap(chunk):
        block = z1o.at[y, part(chunk), zl]
        send(block, block, zls.at[chunk], dev(zl=1 - zl))

    def x_spread(zz, chunk, cond):
        block = held2(x, zz, chunk)
        for side in range(2):
            send(block, block, x1s.at[side, zz, chunk], x_sides[side], cond)
        share2(x, zz, chunk, cond)

    def z_move(chunk):
        here = landing(home(x, chunk // 2), chunk)
        arrived(here, ts.at[chunk], moved[chunk // 2])
        pl.when(jnp.logical_not(moved[chunk // 2]))(local(chunk).wait)
        there = held2(x, zl, chunk)
        for target in (dev(zh=1 - zl, zl=zh), dev(zh=zl, zl=zh)):
            send(here, there, us.at[zl, chunk], target, crossed)
        send(here, z2o.at[4, part(chunk), 0], rs.at[chunk], dev(zh=1 - zh, zl=1 - zl), straight)
        x_spread(zl, chunk, straight)

    def relay(chunk):
        here = z2o.at[4, part(chunk), 0]
        arrived(here, rs.at[chunk], straight)
        send(here, held2(x, 1 - zl, chunk), us.at[1 - zl, chunk], dev(zl=1 - zl), straight)

    def x_direct(chunk):
        arrived(held2(x, 1 - zl, chunk), us.at[1 - zl, chunk])
        x_spread(1 - zl, chunk, None)

    def x_relayed(chunk):
        arrived(held2(x, zl, chunk), us.at[zl, chunk], crossed)
        x_spread(zl, chunk, crossed)

    def y_forward(number, chunk):
        zz = zl if number == 0 else 1 - zl
        for side, source in enumerate((yl, yr)):
            block = z1o.at[source, part(chunk), zz]
            arrived(block, y1s.at[side, number, chunk])
            if chunk % 2 == side:
                send(block, block, y2s.at[number, chunk], y_sides[side])
            share1(source, zz, chunk)

    def x_forward(chunk):
        for zz in range(2):
            for side, source in enumerate((xl, xr)):
                block = held2(source, zz, chunk)
                arrived(block, x1s.at[side, zz, chunk])
                if chunk % 2 == side:
                    send(block, block, x2s.at[zz, chunk], x_sides[side])
                share2(source, zz, chunk)

    def zl_step(chunk):
        arrived(z1o.at[y, part(chunk), 1 - zl], zls.at[chunk])
        y_spread(1, 1 - zl, chunk)
        share1(y, 1 - zl, chunk)

    a, b, c, e = order
    zl_swap(a)
    for chunk in order:
        y_spread(0, zl, chunk)
    for chunk in order:
        z_move(chunk)
    zl_swap(b)
    zl_step(a)
    for chunk in order:
        share1(y, zl, chunk)
    x_direct(a)
    relay(a)
    x_direct(b)
    relay(b)
    zl_swap(c)
    x_direct(c)
    relay(c)
    x_relayed(a)
    zl_swap(e)
    x_direct(e)
    relay(e)
    x_relayed(b)
    y_forward(0, a)
    y_forward(0, b)
    zl_step(b)
    x_relayed(c)
    y_forward(0, c)
    y_forward(0, e)
    zl_step(c)
    x_relayed(e)
    x_forward(a)
    zl_step(e)
    y_forward(1, a)
    x_forward(b)
    y_forward(1, b)
    x_forward(c)
    y_forward(1, c)
    x_forward(e)
    y_forward(1, e)

    size = PIECES // 2

    def slab(ref, yy, s, columns=slice(None)):
        block = ref[yy, pl.ds(s * size, size), :, :, columns]
        return block.reshape(-1, block.shape[-1])

    def accumulate(number, held, yy, s):
        right = slab(z1o, yy, s)
        for start in range(0, depth, tile):
            left = slab(held, yy, s, pl.ds(start, tile))
            acc[number, pl.ds(start, tile), :] += lax.dot_general(
                left, right, (((0,), (0,)), ((), ())), preferred_element_type=F32
            )

    def correlate_own(yy, s):
        accumulate(0, z2o, yy, s)

    def correlate_other(yy, s):
        arrived(z2p.at[yy, pl.ds(s * size, size)], k2s.at[yy, s])
        accumulate(1, z2p, yy, s)

    def correlate(yy, s):
        correlate_own(yy, s)
        correlate_other(yy, s)

    def last_along_y(half):
        return mod4(2 - x + 2 * half)

    def early(step, carry):
        half = step % 2
        late_one = last_along_y(half)
        first = jnp.where(late_one == 0, 1, 0)
        second = jnp.where(late_one < 2, 3, 1)
        correlate(home(mod4(x + jnp.where(step < 2, first, second)), half), half)
        return carry

    acc[...] = jnp.zeros_like(acc)
    lax.fori_loop(0, 4, early, 0)
    for number in range(2):
        zz = zl if number == 0 else 1 - zl
        for chunk in range(CHUNKS):
            arrived(z1o.at[mod4(y + 2), part(chunk), zz], y2s.at[number, chunk])
            share1(mod4(y + 2), zz, chunk)

    def third(step, carry):
        late_one = last_along_y(step)
        correlate(home(mod4(x + jnp.where(late_one == 2, 3, late_one)), step), step)
        return carry

    lax.fori_loop(0, 2, third, 0)
    for chunk in order:
        for zz in range(2):
            arrived(held2(mod4(x + 2), zz, chunk), x2s.at[zz, chunk])
            share2(mod4(x + 2), zz, chunk)

    for part_of in (correlate_own, correlate_other):
        def last(step, carry):
            part_of(home(mod4(x + 2), step), step)
            return carry

        lax.fori_loop(0, 2, last, 0)

    def weigh(number, target):
        half = k if number == 0 else 1 - k
        for start in range(0, depth, tile):
            shape = (tile, depth)
            row_ids = row * (2 * depth) + half * depth + start + lax.broadcasted_iota(jnp.int32, shape, 0)
            col_ids = col * depth + lax.broadcasted_iota(jnp.int32, shape, 1)
            identity = jnp.where(row_ids == col_ids, 1.0, 0.0).astype(F32)
            correlation = acc[number, pl.ds(start, tile), :] / samples
            weights = w[half, pl.ds(start, tile), :].astype(F32)
            target[pl.ds(start, tile), :] = (weights * (correlation - identity)).astype(BF16)

    fetch.wait()
    weigh(1, gp)
    send(gp, gr, gs.at[0], partner)
    weigh(0, go)
    arrived(z1p, k1s.at[0])

    def first_part(yy, s):
        total = jnp.dot(slab(z2o, yy, s), go[...], preferred_element_type=F32)
        total += jnp.dot(slab(z2p, yy, s), gp[...], preferred_element_type=F32)
        p1[yy, pl.ds(s * size, size)] = total.astype(BF16).reshape((size,) + p1.shape[2:])

    def second_part(yy, s, ready=None):
        total = lax.dot_general(slab(z1o, yy, s), go[...], TURNED, preferred_element_type=F32)
        if ready is not None:
            ready()
        total += lax.dot_general(slab(z1p, yy, s), gr[...], TURNED, preferred_element_type=F32)
        p2[yy, pl.ds(s * size, size)] = total.astype(BF16).reshape((size,) + p2.shape[2:])

    def pieces(s):
        return range(s * size, (s + 1) * size)

    def to_far(held, yy, s, far_in, far_sem, sides):
        for p in pieces(s):
            send(held.at[yy, p], far_in.at[p], far_sem.at[p], sides[p % 2])

    def far_x(s, ready=None):
        second_part(home(mod4(x + 2), s), s, ready)
        to_far(p2, home(mod4(x + 2), s), s, rx2, sx2, x_sides)

    def far_y(s):
        first_part(mod4(y + 2), s)
        to_far(p1, mod4(y + 2), s, ry2, sy2, y_sides)

    far_x(0, lambda: arrived(gr, gs.at[0]))
    far_y(0)
    far_x(1)
    far_y(1)

    def to_near(held, ahead, p, far_in, far_sem, near_in, near_sem, sides, which=(0, 1)):
        for side in which:
            yy = ahead[side]
            if p % 2 == side:
                arrived(far_in.at[p], far_sem.at[p])
                held[yy, p] = (held[yy, p].astype(F32) + far_in[p].astype(F32)).astype(BF16)
            send(held.at[yy, p], near_in.at[side, p], near_sem.at[side, p], sides[side])

    def along_x(p, which=(0, 1)):
        to_near(p2, (home(xr, p // size), home(xl, p // size)), p, rx2, sx2, rx1, sx1, x_sides, which)

    def along_y(p, which=(0, 1)):
        to_near(p1, (yr, yl), p, ry2, sy2, ry1, sy1, y_sides, which)

    for s in range(2):
        def near_x(step, carry):
            second_part(home(mod4(x + 1 + 2 * step), s), s)
            return carry

        def near_y(step, carry):
            first_part(mod4(y + 1 + 2 * step), s)
            return carry

        lax.fori_loop(0, 2, near_x, 0)
        if s == 0:
            for p in range(size):
                along_x(p)
        lax.fori_loop(0, 2, near_y, 0)
        if s == 0:
            for p in range(size):
                along_y(p)

    def own(step, carry):
        second_part(home(x, step), step)
        first_part(y, step)
        return carry

    lax.fori_loop(0, 2, own, 0)

    goes = [jnp.logical_or(crossed, zl != zz) for zz in range(2)]

    def x_total(p):
        here = home(x, p // size)
        for side in range(2):
            arrived(rx1.at[side, p], sx1.at[side, p])
        value = p2[here, p].astype(F32) + rx1[0, p].astype(F32) + rx1[1, p].astype(F32)
        p2[here, p] = value.astype(BF16)
        for zz in range(2):
            send(p2.at[here, p, zz], rz.at[zh, p], sz.at[zh, p], dev(zh=zl, zl=zz), goes[zz])

            @pl.when(jnp.logical_not(goes[zz]))
            def _():
                rz[zh, p] = p2[here, p, zz]

    def x_final(p):
        for source in range(2):
            arrived(rz.at[source, p], sz.at[source, p], jnp.logical_or(crossed, zh != source))
        value = (rz[0, p].astype(F32) + rz[1, p].astype(F32)).astype(BF16)
        half = p // size
        fin_out[p] = value
        send(fin_out.at[p], mid.at[p], smid.at[p], dev(y=home(x, half)), moves_y[half])

        @pl.when(jnp.logical_not(moves_y[half]))
        def _():
            mid[p] = value

    def x_onward(p):
        half = p // size
        arrived(mid.at[p], smid.at[p], moves_y[half])
        send(mid.at[p], fin_in.at[p], sfin.at[p], dev(x=mod4(x + y - 2 * half)), moves_x[half])

        @pl.when(jnp.logical_not(moves_x[half]))
        def _():
            o2[p] = mid[p]

    def of_y(p, zz):
        return p1[y, p, zz].astype(F32) + ry1[0, p, zz].astype(F32) + ry1[1, p, zz].astype(F32)

    def y_total(p):
        for side in range(2):
            arrived(ry1.at[side, p], sy1.at[side, p])
        p1[y, p, 1 - zl] = of_y(p, 1 - zl).astype(BF16)
        send(p1.at[y, p, 1 - zl], rzl.at[p], szl.at[p], dev(zl=1 - zl))

    def y_final(p):
        arrived(rzl.at[p], szl.at[p])
        o1[p] = (of_y(p, zl) + rzl[p].astype(F32)).astype(BF16)

    stages = (
        (0, x_total), (-AHEAD, along_x), (LAG, x_final), (-AHEAD, along_y), (1, y_total), (ONWARD, x_onward),
        (Y_LAG, y_final),
    )
    for turn in range(PIECES + max(ONWARD, Y_LAG)):
        for lag, stage in stages:
            if (size if lag < 0 else 0) <= turn - lag < PIECES:
                stage(turn - lag)

    for p in range(PIECES):
        half = p // size
        arrived(fin_in.at[p], sfin.at[p], moves_x[half])

        @pl.when(moves_x[half])
        def _():
            o2[p] = fin_in[p]

    for size, cond, pieces_sent, number in groups:
        ref = gp if size == GROUP else tally.at[pl.ds(0, pieces_sent)]
        copy = pltpu.make_async_remote_copy(
            src_ref=ref, dst_ref=ref, send_sem=ssem.at[number], recv_sem=ssem.at[number],
            device_id=partner, device_id_type=pl.DeviceIdType.MESH,
        )
        if cond is None:
            copy.wait_send()
        else:
            pl.when(cond)(copy.wait_send)


GROUP = 8 * PIECES
SENDS = 17


def per_device(view_one, view_two, pair_weights):
    n = PIECES
    rows, depth = view_one.shape
    piece = (rows // n, depth)
    vmem = lambda *lead: pltpu.VMEM(lead + piece, BF16)
    square = (depth, depth)
    dma = lambda *shape: pltpu.SemaphoreType.DMA(shape)
    cut = (n,) + piece
    flops = 2 * 3 * 8 * rows * 2 * depth * depth
    first, second = pl.pallas_call(
        kernel,
        out_shape=[jax.ShapeDtypeStruct(cut, BF16)] * 2,
        in_specs=[
            pl.BlockSpec(memory_space=pltpu.HBM),
            pl.BlockSpec(memory_space=pltpu.HBM),
            pl.BlockSpec(memory_space=pltpu.HBM),
        ],
        out_specs=[pl.BlockSpec(memory_space=pltpu.VMEM)] * 2,
        scratch_shapes=[
            pltpu.VMEM((2,) + square, BF16),
            vmem(4, n, 2), vmem(4, n, 2), vmem(5, n, 2), vmem(4, n, 2),
            pltpu.VMEM((2,) + square, F32),
            pltpu.VMEM(square, BF16), pltpu.VMEM(square, BF16), pltpu.VMEM(square, BF16),
            vmem(4, n, 2), vmem(4, n, 2),
            vmem(n, 2), vmem(2, n, 2), vmem(2, n),
            vmem(n, 2), vmem(2, n, 2), vmem(n), vmem(n), vmem(n), vmem(n), vmem(GROUP),
            dma(2), dma(SENDS), dma(1), dma(4, 2), dma(CHUNKS), dma(2, 2, CHUNKS), dma(2, CHUNKS),
            dma(CHUNKS), dma(CHUNKS), dma(2, CHUNKS), dma(2, 2, CHUNKS), dma(2, CHUNKS), dma(1),
            dma(n), dma(2, n), dma(2, n), dma(n), dma(2, n), dma(n), dma(n), dma(n),
        ],
        compiler_params=pltpu.CompilerParams(
            collective_id=0, has_side_effects=True, vmem_limit_bytes=53 * 1024 * 1024
        ),
        cost_estimate=pl.CostEstimate(flops=flops, bytes_accessed=8 * rows * depth, transcendentals=0),
    )(view_one.reshape(cut), view_two.reshape(cut), pair_weights.reshape((2,) + square))
    return first.reshape(rows, depth), second.reshape(rows, depth)


def solution(mesh):
    placed = (P("row", "col"),) * 3
    return jax.shard_map(
        per_device, mesh=mesh, in_specs=placed, out_specs=(P("row", "col"),) * 2, check_vma=False
    )
```

```python
import functools

import jax
import jax.numpy as jnp
from jax import lax
from jax.experimental import pallas as pl
from jax.experimental.pallas import tpu as pltpu
from jax.sharding import PartitionSpec as P

F32 = jnp.float32
BF16 = jnp.bfloat16
PIECES = 8
CHUNKS = 4
WIDE = PIECES // CHUNKS
LAG = 2
AHEAD = 3
ONWARD = 5
Y_LAG = 4
TURNED = (((1,), (1,)), ((), ()))


def kernel(
    v1, v2, w_hbm, o1, o2,
    w, z1o, z1p, z2o, z2p, acc, go, gp, gr, p1, p2, rx2, rx1, rz, ry2, ry1, rzl, fin_out, mid, fin_in, tally, staged,
    lsem, ssem, k1s, k2s, zls, y1s, y2s, ts, rs, us, x1s, x2s, gs, sx2, sx1, sz, sy2, sy1, szl, smid, sfin,
):
    row, col = lax.axis_index("row"), lax.axis_index("col")
    y, zl = row // 2, row % 2
    x, zh, k = col // 4, (col // 2) % 2, col % 2
    depth = v1.shape[2]
    samples = v1.shape[0] * v1.shape[1] * 8
    tile = min(256, depth)

    def dev(x=x, y=y, zh=zh, zl=zl, k=k):
        return (y * 2 + zl, x * 4 + zh * 2 + k)

    def mod4(a):
        return (a + 8) % 4

    xr, xl, yr, yl = mod4(x + 1), mod4(x - 1), mod4(y + 1), mod4(y - 1)
    crossed = zh != zl
    straight = zh == zl
    partner = dev(k=1 - k)
    x_sides = (dev(x=xr), dev(x=xl))
    y_sides = (dev(y=yr), dev(y=yl))

    groups = []

    def send(src, dst, recv, where, cond=None):
        size = 1
        for extent in src.shape[:-2]:
            size *= extent
        if len(src.shape) == 2 and src.shape != v1.shape[1:]:
            size = GROUP
        for group in groups:
            if group[0] == size and group[1] is cond and group[2] + size <= GROUP:
                break
        else:
            group = [size, cond, 0, len(groups)]
            groups.append(group)
        group[2] += size
        copy = pltpu.make_async_remote_copy(
            src_ref=src, dst_ref=dst, send_sem=ssem.at[group[3]], recv_sem=recv,
            device_id=where, device_id_type=pl.DeviceIdType.MESH,
        )
        if cond is None:
            copy.start()
        else:
            pl.when(cond)(copy.start)

    def arrived(dst, recv, cond=None):
        copy = pltpu.make_async_remote_copy(
            src_ref=dst, dst_ref=dst, send_sem=ssem.at[0], recv_sem=recv,
            device_id=partner, device_id_type=pl.DeviceIdType.MESH,
        )
        if cond is None:
            copy.wait_recv()
        else:
            pl.when(cond)(copy.wait_recv)

    def home(xx, half):
        return mod4(y - xx + 2 * half)

    t_dest = [dev(x=mod4(x - y + 2 * half), y=x) for half in range(2)]
    t_source = [dev(x=y, y=home(x, half)) for half in range(2)]
    moves_y = [x != 2 * half for half in range(2)]
    moves_x = [y != 2 * half for half in range(2)]
    moved = [jnp.logical_or(moves_x[half], moves_y[half]) for half in range(2)]

    def part(chunk):
        return pl.ds(chunk * WIDE, WIDE)

    load = pltpu.make_async_copy(v1, z1o.at[y, :, zl], lsem.at[0])
    load.start()
    ready = pltpu.make_async_copy(v2, staged, lsem.at[2])
    ready.start()
    fetch = pltpu.make_async_copy(w_hbm, w, lsem.at[1])
    fetch.start()
    barrier = pltpu.get_barrier_semaphore()
    for where in x_sides + y_sides + (
        partner, dev(zl=1 - zl), dev(zh=1 - zh), dev(zh=1 - zh, zl=1 - zl), dev(x=mod4(x + 2)), dev(y=mod4(y + 2)),
    ):
        pl.semaphore_signal(barrier, inc=1, device_id=where, device_id_type=pl.DeviceIdType.MESH)
    for half in range(2):
        @pl.when(moved[half])
        def _():
            for where in (t_dest[half], t_source[half]):
                pl.semaphore_signal(barrier, inc=1, device_id=where, device_id_type=pl.DeviceIdType.MESH)

    own_blocks = jnp.logical_and(x == y, x % 2 == 0)
    pl.semaphore_wait(barrier, jnp.where(own_blocks, 12, 14))

    spare = jnp.where(crossed, 0, zl)

    def landing(yy, chunk):
        return z2o.at[jnp.where(crossed, 4, yy), part(chunk), spare]

    def local(chunk):
        return pltpu.make_async_copy(v2.at[part(chunk)], landing(home(x, chunk // 2), chunk), ts.at[chunk])

    order = (0, 2, 1, 3)
    ready.wait()
    for chunk in order:
        half = chunk // 2
        send(staged.at[part(chunk)], landing(y, chunk), ts.at[chunk], t_dest[half], moved[half])
        pl.when(jnp.logical_not(moved[half]))(local(chunk).start)

    def share1(yy, zz, chunk):
        block = z1o.at[yy, part(chunk), zz]
        send(block, z1p.at[yy, part(chunk), zz], k1s.at[0], partner)

    def share2(xx, zz, chunk, cond=None):
        block = held2(xx, zz, chunk)
        send(block, z2p.at[home(xx, chunk // 2), part(chunk), zz], k2s.at[home(xx, chunk // 2), chunk // 2], partner, cond)

    def held2(xx, zz, chunk):
        return z2o.at[home(xx, chunk // 2), part(chunk), zz]

    load.wait()

    def y_spread(number, zz, chunk):
        block = z1o.at[y, part(chunk), zz]
        for side in range(2):
            send(block, block, y1s.at[side, number, chunk], y_sides[side])

    def zl_swap(chunk):
        block = z1o.at[y, part(chunk), zl]
        send(block, block, zls.at[chunk], dev(zl=1 - zl))

    def x_spread(zz, chunk, cond):
        block = held2(x, zz, chunk)
        for side in range(2):
            send(block, block, x1s.at[side, zz, chunk], x_sides[side], cond)
        share2(x, zz, chunk, cond)

    def z_move(chunk):
        here = landing(home(x, chunk // 2), chunk)
        arrived(here, ts.at[chunk], moved[chunk // 2])
        pl.when(jnp.logical_not(moved[chunk // 2]))(local(chunk).wait)
        there = held2(x, zl, chunk)
        for target in (dev(zh=1 - zl, zl=zh), dev(zh=zl, zl=zh)):
            send(here, there, us.at[zl, chunk], target, crossed)
        send(here, z2o.at[4, part(chunk), 0], rs.at[chunk], dev(zh=1 - zh, zl=1 - zl), straight)
        x_spread(zl, chunk, straight)

    def relay(chunk):
        here = z2o.at[4, part(chunk), 0]
        arrived(here, rs.at[chunk], straight)
        send(here, held2(x, 1 - zl, chunk), us.at[1 - zl, chunk], dev(zl=1 - zl), straight)

    def x_direct(chunk):
        arrived(held2(x, 1 - zl, chunk), us.at[1 - zl, chunk])
        x_spread(1 - zl, chunk, None)

    def x_relayed(chunk):
        arrived(held2(x, zl, chunk), us.at[zl, chunk], crossed)
        x_spread(zl, chunk, crossed)

    def y_forward(number, chunk):
        zz = zl if number == 0 else 1 - zl
        for side, source in enumerate((yl, yr)):
            block = z1o.at[source, part(chunk), zz]
            arrived(block, y1s.at[side, number, chunk])
            if chunk % 2 == side:
                send(block, block, y2s.at[number, chunk], y_sides[side])
            share1(source, zz, chunk)

    def x_forward(chunk):
        for zz in range(2):
            for side, source in enumerate((xl, xr)):
                block = held2(source, zz, chunk)
                arrived(block, x1s.at[side, zz, chunk])
                if chunk % 2 == side:
                    send(block, block, x2s.at[zz, chunk], x_sides[side])
                share2(source, zz, chunk)

    def zl_step(chunk):
        arrived(z1o.at[y, part(chunk), 1 - zl], zls.at[chunk])
        y_spread(1, 1 - zl, chunk)
        share1(y, 1 - zl, chunk)

    a, b, c, e = order
    zl_swap(a)
    for chunk in order:
        y_spread(0, zl, chunk)
    for chunk in order:
        z_move(chunk)
    zl_swap(b)
    zl_step(a)
    for chunk in order:
        share1(y, zl, chunk)
    x_direct(a)
    relay(a)
    x_direct(b)
    relay(b)
    zl_swap(c)
    x_direct(c)
    relay(c)
    x_relayed(a)
    zl_swap(e)
    x_direct(e)
    relay(e)
    x_relayed(b)
    y_forward(0, a)
    y_forward(0, b)
    zl_step(b)
    x_relayed(c)
    y_forward(0, c)
    y_forward(0, e)
    zl_step(c)
    x_relayed(e)
    x_forward(a)
    zl_step(e)
    y_forward(1, a)
    x_forward(b)
    y_forward(1, b)
    x_forward(c)
    y_forward(1, c)
    x_forward(e)
    y_forward(1, e)

    size = PIECES // 2

    def slab(ref, yy, s, columns=slice(None)):
        block = ref[yy, pl.ds(s * size, size), :, :, columns]
        return block.reshape(-1, block.shape[-1])

    def accumulate(number, held, yy, s):
        right = slab(z1o, yy, s)
        for start in range(0, depth, tile):
            left = slab(held, yy, s, pl.ds(start, tile))
            acc[number, pl.ds(start, tile), :] += lax.dot_general(
                left, right, (((0,), (0,)), ((), ())), preferred_element_type=F32
            )

    def correlate_own(yy, s):
        accumulate(0, z2o, yy, s)

    def correlate_other(yy, s):
        arrived(z2p.at[yy, pl.ds(s * size, size)], k2s.at[yy, s])
        accumulate(1, z2p, yy, s)

    def correlate(yy, s):
        correlate_own(yy, s)
        correlate_other(yy, s)

    def last_along_y(half):
        return mod4(2 - x + 2 * half)

    def early(step, carry):
        half = step % 2
        late_one = last_along_y(half)
        first = jnp.where(late_one == 0, 1, 0)
        second = jnp.where(late_one < 2, 3, 1)
        correlate(home(mod4(x + jnp.where(step < 2, first, second)), half), half)
        return carry

    acc[...] = jnp.zeros_like(acc)
    lax.fori_loop(0, 4, early, 0)
    for number in range(2):
        zz = zl if number == 0 else 1 - zl
        for chunk in range(CHUNKS):
            arrived(z1o.at[mod4(y + 2), part(chunk), zz], y2s.at[number, chunk])
            share1(mod4(y + 2), zz, chunk)

    def third(step, carry):
        late_one = last_along_y(step)
        correlate(home(mod4(x + jnp.where(late_one == 2, 3, late_one)), step), step)
        return carry

    lax.fori_loop(0, 2, third, 0)
    for chunk in order:
        for zz in range(2):
            arrived(held2(mod4(x + 2), zz, chunk), x2s.at[zz, chunk])
            share2(mod4(x + 2), zz, chunk)

    for part_of in (correlate_own, correlate_other):
        def last(step, carry):
            part_of(home(mod4(x + 2), step), step)
            return carry

        lax.fori_loop(0, 2, last, 0)

    def weigh(number, target):
        half = k if number == 0 else 1 - k
        for start in range(0, depth, tile):
            shape = (tile, depth)
            row_ids = row * (2 * depth) + half * depth + start + lax.broadcasted_iota(jnp.int32, shape, 0)
            col_ids = col * depth + lax.broadcasted_iota(jnp.int32, shape, 1)
            identity = jnp.where(row_ids == col_ids, 1.0, 0.0).astype(F32)
            correlation = acc[number, pl.ds(start, tile), :] / samples
            weights = w[half, pl.ds(start, tile), :].astype(F32)
            target[pl.ds(start, tile), :] = (weights * (correlation - identity)).astype(BF16)

    fetch.wait()
    weigh(1, gp)
    send(gp, gr, gs.at[0], partner)
    weigh(0, go)
    arrived(z1p, k1s.at[0])

    def first_part(yy, s):
        total = jnp.dot(slab(z2o, yy, s), go[...], preferred_element_type=F32)
        total += jnp.dot(slab(z2p, yy, s), gp[...], preferred_element_type=F32)
        p1[yy, pl.ds(s * size, size)] = total.astype(BF16).reshape((size,) + p1.shape[2:])

    def second_part(yy, s, ready=None):
        total = lax.dot_general(slab(z1o, yy, s), go[...], TURNED, preferred_element_type=F32)
        if ready is not None:
            ready()
        total += lax.dot_general(slab(z1p, yy, s), gr[...], TURNED, preferred_element_type=F32)
        p2[yy, pl.ds(s * size, size)] = total.astype(BF16).reshape((size,) + p2.shape[2:])

    def pieces(s):
        return range(s * size, (s + 1) * size)

    def to_far(held, yy, s, far_in, far_sem, sides):
        for p in pieces(s):
            send(held.at[yy, p], far_in.at[p], far_sem.at[p], sides[p % 2])

    def far_x(s, ready=None):
        second_part(home(mod4(x + 2), s), s, ready)
        to_far(p2, home(mod4(x + 2), s), s, rx2, sx2, x_sides)

    def far_y(s):
        first_part(mod4(y + 2), s)
        to_far(p1, mod4(y + 2), s, ry2, sy2, y_sides)

    far_x(0, lambda: arrived(gr, gs.at[0]))
    far_y(0)
    far_x(1)
    far_y(1)

    def to_near(held, ahead, p, far_in, far_sem, near_in, near_sem, sides, which=(0, 1)):
        for side in which:
            yy = ahead[side]
            if p % 2 == side:
                arrived(far_in.at[p], far_sem.at[p])
                held[yy, p] = (held[yy, p].astype(F32) + far_in[p].astype(F32)).astype(BF16)
            send(held.at[yy, p], near_in.at[side, p], near_sem.at[side, p], sides[side])

    def along_x(p, which=(0, 1)):
        to_near(p2, (home(xr, p // size), home(xl, p // size)), p, rx2, sx2, rx1, sx1, x_sides, which)

    def along_y(p, which=(0, 1)):
        to_near(p1, (yr, yl), p, ry2, sy2, ry1, sy1, y_sides, which)

    for s in range(2):
        def near_x(step, carry):
            second_part(home(mod4(x + 1 + 2 * step), s), s)
            return carry

        def near_y(step, carry):
            first_part(mod4(y + 1 + 2 * step), s)
            return carry

        lax.fori_loop(0, 2, near_x, 0)
        if s == 0:
            for p in range(size):
                along_x(p)
        lax.fori_loop(0, 2, near_y, 0)
        if s == 0:
            for p in range(size):
                along_y(p)

    def own(step, carry):
        second_part(home(x, step), step)
        first_part(y, step)
        return carry

    lax.fori_loop(0, 2, own, 0)

    goes = [jnp.logical_or(crossed, zl != zz) for zz in range(2)]

    def x_total(p):
        here = home(x, p // size)
        for side in range(2):
            arrived(rx1.at[side, p], sx1.at[side, p])
        value = p2[here, p].astype(F32) + rx1[0, p].astype(F32) + rx1[1, p].astype(F32)
        p2[here, p] = value.astype(BF16)
        for zz in range(2):
            send(p2.at[here, p, zz], rz.at[zh, p], sz.at[zh, p], dev(zh=zl, zl=zz), goes[zz])

            @pl.when(jnp.logical_not(goes[zz]))
            def _():
                rz[zh, p] = p2[here, p, zz]

    def x_final(p):
        for source in range(2):
            arrived(rz.at[source, p], sz.at[source, p], jnp.logical_or(crossed, zh != source))
        value = (rz[0, p].astype(F32) + rz[1, p].astype(F32)).astype(BF16)
        half = p // size
        fin_out[p] = value
        send(fin_out.at[p], mid.at[p], smid.at[p], dev(y=home(x, half)), moves_y[half])

        @pl.when(jnp.logical_not(moves_y[half]))
        def _():
            mid[p] = value

    def x_onward(p):
        half = p // size
        arrived(mid.at[p], smid.at[p], moves_y[half])
        send(mid.at[p], fin_in.at[p], sfin.at[p], dev(x=mod4(x + y - 2 * half)), moves_x[half])

        @pl.when(jnp.logical_not(moves_x[half]))
        def _():
            o2[p] = mid[p]

    def of_y(p, zz):
        return p1[y, p, zz].astype(F32) + ry1[0, p, zz].astype(F32) + ry1[1, p, zz].astype(F32)

    def y_total(p):
        for side in range(2):
            arrived(ry1.at[side, p], sy1.at[side, p])
        p1[y, p, 1 - zl] = of_y(p, 1 - zl).astype(BF16)
        send(p1.at[y, p, 1 - zl], rzl.at[p], szl.at[p], dev(zl=1 - zl))

    def y_final(p):
        arrived(rzl.at[p], szl.at[p])
        o1[p] = (of_y(p, zl) + rzl[p].astype(F32)).astype(BF16)

    stages = (
        (0, x_total), (-AHEAD, along_x), (LAG, x_final), (-AHEAD, along_y), (1, y_total), (ONWARD, x_onward),
        (Y_LAG, y_final),
    )
    for turn in range(PIECES + max(ONWARD, Y_LAG)):
        for lag, stage in stages:
            if (size if lag < 0 else 0) <= turn - lag < PIECES:
                stage(turn - lag)

    for p in range(PIECES):
        half = p // size
        arrived(fin_in.at[p], sfin.at[p], moves_x[half])

        @pl.when(moves_x[half])
        def _():
            o2[p] = fin_in[p]

    for size, cond, pieces_sent, number in groups:
        ref = gp if size == GROUP else tally.at[pl.ds(0, pieces_sent)]
        copy = pltpu.make_async_remote_copy(
            src_ref=ref, dst_ref=ref, send_sem=ssem.at[number], recv_sem=ssem.at[number],
            device_id=partner, device_id_type=pl.DeviceIdType.MESH,
        )
        if cond is None:
            copy.wait_send()
        else:
            pl.when(cond)(copy.wait_send)


GROUP = 8 * PIECES
SENDS = 17


def per_device(view_one, view_two, pair_weights):
    n = PIECES
    rows, depth = view_one.shape
    piece = (rows // n, depth)
    vmem = lambda *lead: pltpu.VMEM(lead + piece, BF16)
    square = (depth, depth)
    dma = lambda *shape: pltpu.SemaphoreType.DMA(shape)
    cut = (n,) + piece
    flops = 2 * 3 * 8 * rows * 2 * depth * depth
    first, second = pl.pallas_call(
        kernel,
        out_shape=[jax.ShapeDtypeStruct(cut, BF16)] * 2,
        in_specs=[
            pl.BlockSpec(memory_space=pltpu.HBM),
            pl.BlockSpec(memory_space=pltpu.HBM),
            pl.BlockSpec(memory_space=pltpu.HBM),
        ],
        out_specs=[pl.BlockSpec(memory_space=pltpu.VMEM)] * 2,
        scratch_shapes=[
            pltpu.VMEM((2,) + square, BF16),
            vmem(4, n, 2), vmem(4, n, 2), vmem(5, n, 2), vmem(4, n, 2),
            pltpu.VMEM((2,) + square, F32),
            pltpu.VMEM(square, BF16), pltpu.VMEM(square, BF16), pltpu.VMEM(square, BF16),
            vmem(4, n, 2), vmem(4, n, 2),
            vmem(n, 2), vmem(2, n, 2), vmem(2, n),
            vmem(n, 2), vmem(2, n, 2), vmem(n), vmem(n), vmem(n), vmem(n), vmem(GROUP), vmem(n),
            dma(3), dma(SENDS), dma(1), dma(4, 2), dma(CHUNKS), dma(2, 2, CHUNKS), dma(2, CHUNKS),
            dma(CHUNKS), dma(CHUNKS), dma(2, CHUNKS), dma(2, 2, CHUNKS), dma(2, CHUNKS), dma(1),
            dma(n), dma(2, n), dma(2, n), dma(n), dma(2, n), dma(n), dma(n), dma(n),
        ],
        compiler_params=pltpu.CompilerParams(
            collective_id=0, has_side_effects=True, vmem_limit_bytes=53 * 1024 * 1024
        ),
        cost_estimate=pl.CostEstimate(flops=flops, bytes_accessed=8 * rows * depth, transcendentals=0),
    )(view_one.reshape(cut), view_two.reshape(cut), pair_weights.reshape((2,) + square))
    return first.reshape(rows, depth), second.reshape(rows, depth)


def solution(mesh):
    placed = (P("row", "col"),) * 3
    return jax.shard_map(
        per_device, mesh=mesh, in_specs=placed, out_specs=(P("row", "col"),) * 2, check_vma=False
    )
```

```python
import functools

import jax
import jax.numpy as jnp
from jax import lax
from jax.experimental import pallas as pl
from jax.experimental.pallas import tpu as pltpu
from jax.sharding import PartitionSpec as P

F32 = jnp.float32
BF16 = jnp.bfloat16
PIECES = 8
CHUNKS = 4
WIDE = PIECES // CHUNKS
LAG = 2
AHEAD = 3
ONWARD = 5
Y_LAG = 4
TURNED = (((1,), (1,)), ((), ()))


def kernel(
    v1, v2, w_hbm, o1, o2,
    w, z1o, z1p, z2o, z2p, acc, go, gp, gr, p1, p2, rx2, rx1, rz, ry2, ry1, rzl, fin_out, mid, fin_in, tally, staged,
    lsem, ssem, k1s, k2s, zls, y1s, y2s, ts, rs, us, x1s, x2s, gs, sx2, sx1, sz, sy2, sy1, szl, smid, sfin,
):
    row, col = lax.axis_index("row"), lax.axis_index("col")
    y, zl = row // 2, row % 2
    x, zh, k = col // 4, (col // 2) % 2, col % 2
    depth = v1.shape[2]
    samples = v1.shape[0] * v1.shape[1] * 8
    tile = min(256, depth)

    def dev(x=x, y=y, zh=zh, zl=zl, k=k):
        return (y * 2 + zl, x * 4 + zh * 2 + k)

    def mod4(a):
        return (a + 8) % 4

    xr, xl, yr, yl = mod4(x + 1), mod4(x - 1), mod4(y + 1), mod4(y - 1)
    crossed = zh != zl
    straight = zh == zl
    partner = dev(k=1 - k)
    x_sides = (dev(x=xr), dev(x=xl))
    y_sides = (dev(y=yr), dev(y=yl))

    groups = []

    def send(src, dst, recv, where, cond=None):
        size = 1
        for extent in src.shape[:-2]:
            size *= extent
        if len(src.shape) == 2 and src.shape != v1.shape[1:]:
            size = GROUP
        for group in groups:
            if group[0] == size and group[1] is cond and group[2] + size <= GROUP:
                break
        else:
            group = [size, cond, 0, len(groups)]
            groups.append(group)
        group[2] += size
        copy = pltpu.make_async_remote_copy(
            src_ref=src, dst_ref=dst, send_sem=ssem.at[group[3]], recv_sem=recv,
            device_id=where, device_id_type=pl.DeviceIdType.MESH,
        )
        if cond is None:
            copy.start()
        else:
            pl.when(cond)(copy.start)

    def arrived(dst, recv, cond=None):
        copy = pltpu.make_async_remote_copy(
            src_ref=dst, dst_ref=dst, send_sem=ssem.at[0], recv_sem=recv,
            device_id=partner, device_id_type=pl.DeviceIdType.MESH,
        )
        if cond is None:
            copy.wait_recv()
        else:
            pl.when(cond)(copy.wait_recv)

    def home(xx, half):
        return mod4(y - xx + 2 * half)

    t_dest = [dev(x=mod4(x - y + 2 * half), y=x) for half in range(2)]
    t_source = [dev(x=y, y=home(x, half)) for half in range(2)]
    moves_y = [x != 2 * half for half in range(2)]
    moves_x = [y != 2 * half for half in range(2)]
    moved = [jnp.logical_or(moves_x[half], moves_y[half]) for half in range(2)]

    def part(chunk):
        return pl.ds(chunk * WIDE, WIDE)

    load = pltpu.make_async_copy(v1, z1o.at[y, :, zl], lsem.at[0])
    load.start()
    ready = pltpu.make_async_copy(v2, staged, lsem.at[2])
    ready.start()
    fetch = pltpu.make_async_copy(w_hbm, w, lsem.at[1])
    fetch.start()
    barrier = pltpu.get_barrier_semaphore()
    for where in x_sides + y_sides + (
        partner, dev(zl=1 - zl), dev(zh=1 - zh), dev(zh=1 - zh, zl=1 - zl), dev(x=mod4(x + 2)), dev(y=mod4(y + 2)),
    ):
        pl.semaphore_signal(barrier, inc=1, device_id=where, device_id_type=pl.DeviceIdType.MESH)
    for half in range(2):
        @pl.when(moved[half])
        def _():
            for where in (t_dest[half], t_source[half]):
                pl.semaphore_signal(barrier, inc=1, device_id=where, device_id_type=pl.DeviceIdType.MESH)

    own_blocks = jnp.logical_and(x == y, x % 2 == 0)
    pl.semaphore_wait(barrier, jnp.where(own_blocks, 12, 14))

    spare = jnp.where(crossed, 0, zl)

    def landing(yy, chunk):
        return z2o.at[jnp.where(crossed, 4, yy), part(chunk), spare]

    def local(chunk):
        return pltpu.make_async_copy(v2.at[part(chunk)], landing(home(x, chunk // 2), chunk), ts.at[chunk])

    order = (0, 2, 1, 3)
    ready.wait()
    for chunk in order:
        half = chunk // 2
        send(staged.at[part(chunk)], landing(y, chunk), ts.at[chunk], t_dest[half], moved[half])
        pl.when(jnp.logical_not(moved[half]))(local(chunk).start)

    def share1(yy, zz, chunk):
        block = z1o.at[yy, part(chunk), zz]
        send(block, z1p.at[yy, part(chunk), zz], k1s.at[0], partner)

    def share2(xx, zz, chunk, cond=None):
        block = held2(xx, zz, chunk)
        send(block, z2p.at[home(xx, chunk // 2), part(chunk), zz], k2s.at[home(xx, chunk // 2), chunk // 2], partner, cond)

    def held2(xx, zz, chunk):
        return z2o.at[home(xx, chunk // 2), part(chunk), zz]

    load.wait()

    def y_spread(number, zz, chunk):
        block = z1o.at[y, part(chunk), zz]
        for side in range(2):
            send(block, block, y1s.at[side, number, chunk], y_sides[side])

    def zl_swap(chunk):
        block = z1o.at[y, part(chunk), zl]
        send(block, block, zls.at[chunk], dev(zl=1 - zl))

    def x_spread(zz, chunk, cond):
        block = held2(x, zz, chunk)
        for side in range(2):
            send(block, block, x1s.at[side, zz, chunk], x_sides[side], cond)
        share2(x, zz, chunk, cond)

    def z_move(chunk):
        here = landing(home(x, chunk // 2), chunk)
        arrived(here, ts.at[chunk], moved[chunk // 2])
        pl.when(jnp.logical_not(moved[chunk // 2]))(local(chunk).wait)
        there = held2(x, zl, chunk)
        for target in (dev(zh=1 - zl, zl=zh), dev(zh=zl, zl=zh)):
            send(here, there, us.at[zl, chunk], target, crossed)
        send(here, z2o.at[4, part(chunk), 0], rs.at[chunk], dev(zh=1 - zh, zl=1 - zl), straight)
        x_spread(zl, chunk, straight)

    def relay(chunk):
        here = z2o.at[4, part(chunk), 0]
        arrived(here, rs.at[chunk], straight)
        send(here, held2(x, 1 - zl, chunk), us.at[1 - zl, chunk], dev(zl=1 - zl), straight)

    def x_direct(chunk):
        arrived(held2(x, 1 - zl, chunk), us.at[1 - zl, chunk])
        x_spread(1 - zl, chunk, None)

    def x_relayed(chunk):
        arrived(held2(x, zl, chunk), us.at[zl, chunk], crossed)
        x_spread(zl, chunk, crossed)

    def y_forward(number, chunk):
        zz = zl if number == 0 else 1 - zl
        for side, source in enumerate((yl, yr)):
            block = z1o.at[source, part(chunk), zz]
            arrived(block, y1s.at[side, number, chunk])
            if chunk % 2 == side:
                send(block, block, y2s.at[number, chunk], y_sides[side])
            share1(source, zz, chunk)

    def x_forward(chunk):
        for zz in range(2):
            for side, source in enumerate((xl, xr)):
                block = held2(source, zz, chunk)
                arrived(block, x1s.at[side, zz, chunk])
                if chunk % 2 == side:
                    send(block, block, x2s.at[zz, chunk], x_sides[side])
                share2(source, zz, chunk)

    def zl_step(chunk):
        arrived(z1o.at[y, part(chunk), 1 - zl], zls.at[chunk])
        y_spread(1, 1 - zl, chunk)
        share1(y, 1 - zl, chunk)

    a, b, c, e = order
    zl_swap(a)
    for chunk in order:
        y_spread(0, zl, chunk)
    for chunk in order:
        z_move(chunk)
    zl_swap(b)
    zl_step(a)
    for chunk in order:
        share1(y, zl, chunk)
    x_direct(a)
    relay(a)
    x_direct(b)
    relay(b)
    zl_swap(c)
    x_direct(c)
    relay(c)
    x_relayed(a)
    zl_swap(e)
    x_direct(e)
    relay(e)
    x_relayed(b)
    y_forward(0, a)
    y_forward(0, b)
    zl_step(b)
    x_relayed(c)
    y_forward(0, c)
    y_forward(0, e)
    zl_step(c)
    x_relayed(e)
    x_forward(a)
    zl_step(e)
    y_forward(1, a)
    x_forward(b)
    y_forward(1, b)
    x_forward(c)
    y_forward(1, c)
    x_forward(e)
    y_forward(1, e)

    size = PIECES // 2

    def slab(ref, yy, s, columns=slice(None)):
        block = ref[yy, pl.ds(s * size, size), :, :, columns]
        return block.reshape(-1, block.shape[-1])

    def accumulate(number, held, yy, s):
        right = slab(z1o, yy, s)
        for start in range(0, depth, tile):
            left = slab(held, yy, s, pl.ds(start, tile))
            acc[number, pl.ds(start, tile), :] += lax.dot_general(
                left, right, (((0,), (0,)), ((), ())), preferred_element_type=F32
            )

    def correlate_own(yy, s):
        accumulate(0, z2o, yy, s)

    def correlate_other(yy, s):
        arrived(z2p.at[yy, pl.ds(s * size, size)], k2s.at[yy, s])
        accumulate(1, z2p, yy, s)

    def correlate(yy, s):
        correlate_own(yy, s)
        correlate_other(yy, s)

    def last_along_y(half):
        return mod4(2 - x + 2 * half)

    def early(step, carry):
        half = step % 2
        late_one = last_along_y(half)
        first = jnp.where(late_one == 0, 1, 0)
        second = jnp.where(late_one < 2, 3, 1)
        correlate(home(mod4(x + jnp.where(step < 2, first, second)), half), half)
        return carry

    acc[...] = jnp.zeros_like(acc)
    lax.fori_loop(0, 4, early, 0)
    for number in range(2):
        zz = zl if number == 0 else 1 - zl
        for chunk in range(CHUNKS):
            arrived(z1o.at[mod4(y + 2), part(chunk), zz], y2s.at[number, chunk])
            share1(mod4(y + 2), zz, chunk)

    def third(step, carry):
        late_one = last_along_y(step)
        correlate(home(mod4(x + jnp.where(late_one == 2, 3, late_one)), step), step)
        return carry

    lax.fori_loop(0, 2, third, 0)
    for chunk in order:
        for zz in range(2):
            arrived(held2(mod4(x + 2), zz, chunk), x2s.at[zz, chunk])
            share2(mod4(x + 2), zz, chunk)

    far_columns = [home(mod4(x + 2), half) for half in range(2)]
    correlate_own(far_columns[0], 0)
    correlate_other(far_columns[0], 0)
    correlate_other(far_columns[1], 1)

    def weigh(number, target):
        half = k if number == 0 else 1 - k
        for start in range(0, depth, tile):
            shape = (tile, depth)
            row_ids = row * (2 * depth) + half * depth + start + lax.broadcasted_iota(jnp.int32, shape, 0)
            col_ids = col * depth + lax.broadcasted_iota(jnp.int32, shape, 1)
            identity = jnp.where(row_ids == col_ids, 1.0, 0.0).astype(F32)
            correlation = acc[number, pl.ds(start, tile), :] / samples
            weights = w[half, pl.ds(start, tile), :].astype(F32)
            target[pl.ds(start, tile), :] = (weights * (correlation - identity)).astype(BF16)

    fetch.wait()
    weigh(1, gp)
    send(gp, gr, gs.at[0], partner)
    correlate_own(far_columns[1], 1)
    weigh(0, go)
    arrived(z1p, k1s.at[0])

    def first_part(yy, s):
        total = jnp.dot(slab(z2o, yy, s), go[...], preferred_element_type=F32)
        total += jnp.dot(slab(z2p, yy, s), gp[...], preferred_element_type=F32)
        p1[yy, pl.ds(s * size, size)] = total.astype(BF16).reshape((size,) + p1.shape[2:])

    def second_part(yy, s, ready=None):
        total = lax.dot_general(slab(z1o, yy, s), go[...], TURNED, preferred_element_type=F32)
        if ready is not None:
            ready()
        total += lax.dot_general(slab(z1p, yy, s), gr[...], TURNED, preferred_element_type=F32)
        p2[yy, pl.ds(s * size, size)] = total.astype(BF16).reshape((size,) + p2.shape[2:])

    def pieces(s):
        return range(s * size, (s + 1) * size)

    def to_far(held, yy, s, far_in, far_sem, sides):
        for p in pieces(s):
            send(held.at[yy, p], far_in.at[p], far_sem.at[p], sides[p % 2])

    def far_x(s, ready=None):
        second_part(home(mod4(x + 2), s), s, ready)
        to_far(p2, home(mod4(x + 2), s), s, rx2, sx2, x_sides)

    def far_y(s):
        first_part(mod4(y + 2), s)
        to_far(p1, mod4(y + 2), s, ry2, sy2, y_sides)

    far_x(0, lambda: arrived(gr, gs.at[0]))
    far_y(0)
    far_x(1)
    far_y(1)

    def to_near(held, ahead, p, far_in, far_sem, near_in, near_sem, sides, which=(0, 1)):
        for side in which:
            yy = ahead[side]
            if p % 2 == side:
                arrived(far_in.at[p], far_sem.at[p])
                held[yy, p] = (held[yy, p].astype(F32) + far_in[p].astype(F32)).astype(BF16)
            send(held.at[yy, p], near_in.at[side, p], near_sem.at[side, p], sides[side])

    def along_x(p, which=(0, 1)):
        to_near(p2, (home(xr, p // size), home(xl, p // size)), p, rx2, sx2, rx1, sx1, x_sides, which)

    def along_y(p, which=(0, 1)):
        to_near(p1, (yr, yl), p, ry2, sy2, ry1, sy1, y_sides, which)

    for s in range(2):
        def near_x(step, carry):
            second_part(home(mod4(x + 1 + 2 * step), s), s)
            return carry

        def near_y(step, carry):
            first_part(mod4(y + 1 + 2 * step), s)
            return carry

        lax.fori_loop(0, 2, near_x, 0)
        if s == 0:
            for p in range(size):
                along_x(p)
        lax.fori_loop(0, 2, near_y, 0)
        if s == 0:
            for p in range(size):
                along_y(p)

    def own(step, carry):
        second_part(home(x, step), step)
        first_part(y, step)
        return carry

    lax.fori_loop(0, 2, own, 0)

    goes = [jnp.logical_or(crossed, zl != zz) for zz in range(2)]

    def x_total(p):
        here = home(x, p // size)
        for side in range(2):
            arrived(rx1.at[side, p], sx1.at[side, p])
        value = p2[here, p].astype(F32) + rx1[0, p].astype(F32) + rx1[1, p].astype(F32)
        p2[here, p] = value.astype(BF16)
        for zz in range(2):
            send(p2.at[here, p, zz], rz.at[zh, p], sz.at[zh, p], dev(zh=zl, zl=zz), goes[zz])

            @pl.when(jnp.logical_not(goes[zz]))
            def _():
                rz[zh, p] = p2[here, p, zz]

    def x_final(p):
        for source in range(2):
            arrived(rz.at[source, p], sz.at[source, p], jnp.logical_or(crossed, zh != source))
        value = (rz[0, p].astype(F32) + rz[1, p].astype(F32)).astype(BF16)
        half = p // size
        fin_out[p] = value
        send(fin_out.at[p], mid.at[p], smid.at[p], dev(y=home(x, half)), moves_y[half])

        @pl.when(jnp.logical_not(moves_y[half]))
        def _():
            mid[p] = value

    def x_onward(p):
        half = p // size
        arrived(mid.at[p], smid.at[p], moves_y[half])
        send(mid.at[p], fin_in.at[p], sfin.at[p], dev(x=mod4(x + y - 2 * half)), moves_x[half])

        @pl.when(jnp.logical_not(moves_x[half]))
        def _():
            o2[p] = mid[p]

    def of_y(p, zz):
        return p1[y, p, zz].astype(F32) + ry1[0, p, zz].astype(F32) + ry1[1, p, zz].astype(F32)

    def y_total(p):
        for side in range(2):
            arrived(ry1.at[side, p], sy1.at[side, p])
        p1[y, p, 1 - zl] = of_y(p, 1 - zl).astype(BF16)
        send(p1.at[y, p, 1 - zl], rzl.at[p], szl.at[p], dev(zl=1 - zl))

    def y_final(p):
        arrived(rzl.at[p], szl.at[p])
        o1[p] = (of_y(p, zl) + rzl[p].astype(F32)).astype(BF16)

    stages = (
        (0, x_total), (-AHEAD, along_x), (LAG, x_final), (-AHEAD, along_y), (1, y_total), (ONWARD, x_onward),
        (Y_LAG, y_final),
    )
    for turn in range(PIECES + max(ONWARD, Y_LAG)):
        for lag, stage in stages:
            if (size if lag < 0 else 0) <= turn - lag < PIECES:
                stage(turn - lag)

    for p in range(PIECES):
        half = p // size
        arrived(fin_in.at[p], sfin.at[p], moves_x[half])

        @pl.when(moves_x[half])
        def _():
            o2[p] = fin_in[p]

    for size, cond, pieces_sent, number in groups:
        ref = gp if size == GROUP else tally.at[pl.ds(0, pieces_sent)]
        copy = pltpu.make_async_remote_copy(
            src_ref=ref, dst_ref=ref, send_sem=ssem.at[number], recv_sem=ssem.at[number],
            device_id=partner, device_id_type=pl.DeviceIdType.MESH,
        )
        if cond is None:
            copy.wait_send()
        else:
            pl.when(cond)(copy.wait_send)


GROUP = 8 * PIECES
SENDS = 17


def per_device(view_one, view_two, pair_weights):
    n = PIECES
    rows, depth = view_one.shape
    piece = (rows // n, depth)
    vmem = lambda *lead: pltpu.VMEM(lead + piece, BF16)
    square = (depth, depth)
    dma = lambda *shape: pltpu.SemaphoreType.DMA(shape)
    cut = (n,) + piece
    flops = 2 * 3 * 8 * rows * 2 * depth * depth
    first, second = pl.pallas_call(
        kernel,
        out_shape=[jax.ShapeDtypeStruct(cut, BF16)] * 2,
        in_specs=[
            pl.BlockSpec(memory_space=pltpu.HBM),
            pl.BlockSpec(memory_space=pltpu.HBM),
            pl.BlockSpec(memory_space=pltpu.HBM),
        ],
        out_specs=[pl.BlockSpec(memory_space=pltpu.VMEM)] * 2,
        scratch_shapes=[
            pltpu.VMEM((2,) + square, BF16),
            vmem(4, n, 2), vmem(4, n, 2), vmem(5, n, 2), vmem(4, n, 2),
            pltpu.VMEM((2,) + square, F32),
            pltpu.VMEM(square, BF16), pltpu.VMEM(square, BF16), pltpu.VMEM(square, BF16),
            vmem(4, n, 2), vmem(4, n, 2),
            vmem(n, 2), vmem(2, n, 2), vmem(2, n),
            vmem(n, 2), vmem(2, n, 2), vmem(n), vmem(n), vmem(n), vmem(n), vmem(GROUP), vmem(n),
            dma(3), dma(SENDS), dma(1), dma(4, 2), dma(CHUNKS), dma(2, 2, CHUNKS), dma(2, CHUNKS),
            dma(CHUNKS), dma(CHUNKS), dma(2, CHUNKS), dma(2, 2, CHUNKS), dma(2, CHUNKS), dma(1),
            dma(n), dma(2, n), dma(2, n), dma(n), dma(2, n), dma(n), dma(n), dma(n),
        ],
        compiler_params=pltpu.CompilerParams(
            collective_id=0, has_side_effects=True, vmem_limit_bytes=53 * 1024 * 1024
        ),
        cost_estimate=pl.CostEstimate(flops=flops, bytes_accessed=8 * rows * depth, transcendentals=0),
    )(view_one.reshape(cut), view_two.reshape(cut), pair_weights.reshape((2,) + square))
    return first.reshape(rows, depth), second.reshape(rows, depth)


def solution(mesh):
    placed = (P("row", "col"),) * 3
    return jax.shard_map(
        per_device, mesh=mesh, in_specs=placed, out_specs=(P("row", "col"),) * 2, check_vma=False
    )
```
